512 devices in a mesh: ens: 32 (over z_hi, y, core), lat: 4 (over z_lo), lon: 4 (over x).
Axes of the slice: x: 4, y: 8, z: 8 (z_hi: 2, z_lo: 4; z = z_hi * 4 + z_lo), core: 2. Of those that a mesh axis runs over, the one named last changes fastest.
Arguments:
- sample_quantities: bfloat16 [32, 24, 256, 512], P('ens', None, 'lat', 'lon'), may hold values from -6 to 6
- conv_weight: bfloat16 [216, 256], replicated, may hold values from -0.4375 to 0.4375
- conv_bias: float32 [256], replicated, may hold values from -3 to 3
- out_weight: bfloat16 [256, 24], replicated, may hold values from -0.375 to 0.375
- obs_index: int32 [4, 4, 256], P('lat', 'lon'), may hold values from 0 to 196607
- obs_count: int32 [4, 4], P('lat', 'lon'), may hold values from 85 to 256, as said below
- obs_value: float32 [4, 4, 256], P('lat', 'lon'), may hold values from -8 to 8
- obs_weight: float32 [4, 4, 256], P('lat', 'lon'), may hold values from 0.002 to 0.03
Outputs:
- updated_estimates: bfloat16 [32, 24, 256, 512], P('ens', None, 'lat', 'lon')
The draws below stay inside these ranges and needn't reach their ends.
Inputs may be any that keep to these rules, and one draw needn't show every extreme that they name: `obs_index`: flat index v * 64 * 128 + r * 128 + c into the own shard's block; slots at or past the shard's count are unused. `obs_count`: some shard has exactly 256 live slots.
All inputs are finite; a program needn't handle non-finite values.
Results may differ from the reference program's by a relative error of at most 0.0075.
Values may be sent and summed in bfloat16 or wider, within the bound.
A program may use at most 64 MiB of HBM per device.

```python
import math
import jax
import jax.numpy as jnp
from jax import lax

EVOLVED_QUANTITY = 24
HID = 256
PARALLEL_LINES = 64
MERIDIAN_LINES = 128
OBS_DEV = 256
NS_ITERS = 20
MEMBERS = 32
NLAT = 256
NLON = 512
N_LAT = 4
N_LON = 4


def draw_obs_count(key, part):
    first, second = jax.random.split(jax.random.fold_in(key, 11))
    shards = N_LAT * N_LON
    counts = jax.random.randint(first, (shards,), OBS_DEV // 3, OBS_DEV + 1)
    chosen = jax.random.randint(second, (), 0, shards)
    counts = jnp.where(jnp.arange(shards) == chosen, OBS_DEV, counts)
    return counts.reshape(N_LAT, N_LON).astype(jnp.int32)


def with_ends(result, stream_key, smallest, top_value):
    index_at = [jax.random.randint(jax.random.fold_in(stream_key, axis), (), 0, length) for axis, length in enumerate(result.shape)]
    widest = result.shape.index(max(result.shape))
    beside = index_at[:widest] + [(index_at[widest] + 1) % result.shape[widest]] + index_at[widest + 1:]
    return result.at[tuple(index_at)].set(smallest).at[tuple(beside)].set(top_value)


def steps_of(own_key, shape, cuts, low, top_value):
    gain, own = 1.0, jax.random.fold_in(own_key, 6)
    for axis_at, shards_of in cuts:
        steps = jnp.exp(jax.random.uniform(jax.random.fold_in(own, axis_at), (shards_of,), jnp.float32, low / len(cuts), top_value / len(cuts)))
        gain = gain * jnp.repeat(steps, shape[axis_at] // shards_of).reshape([-1 if axis == axis_at else 1 for axis in range(len(shape))])
    return gain


def centred(key, shape, width, reach, cuts=(), kind=jnp.bfloat16):
    entries = jax.random.normal(key, shape, jnp.float32) * width
    if len(cuts) > 0:
        entries = steps_of(key, shape, cuts, -0.22, 0.18) * entries
    return jnp.clip(entries, min=-reach, max=reach).astype(kind)


def setup_inputs(seed: int = 0) -> dict:
    seeds = jax.random.split(jax.random.key(seed), 9)
    sample_quantities = centred(seeds[0], (MEMBERS, EVOLVED_QUANTITY, NLAT, NLON), 1.0, 6.0, ((0, 32), (2, 4), (3, 4)))
    conv_weight = centred(seeds[1], (9 * EVOLVED_QUANTITY, HID), (9 * EVOLVED_QUANTITY) ** -0.5, 0.4375)
    conv_bias = centred(seeds[2], (HID,), 0.5, 3.0, (), jnp.float32)
    out_weight = centred(seeds[3], (HID, EVOLVED_QUANTITY), HID ** -0.5, 0.375)
    obs_index = with_ends(jax.random.randint(seeds[4], (N_LAT, N_LON, OBS_DEV), 0, EVOLVED_QUANTITY * PARALLEL_LINES * MERIDIAN_LINES), jax.random.fold_in(seeds[4], 1), 0, (EVOLVED_QUANTITY * PARALLEL_LINES * MERIDIAN_LINES) - 1).astype(jnp.int32)
    obs_count = draw_obs_count(jax.random.fold_in(seeds[8], 71), 0)
    obs_value = centred(seeds[6], (N_LAT, N_LON, OBS_DEV), 1.5, 8.0, ((0, 4), (1, 4)), jnp.float32)
    obs_weight = jnp.clip(jnp.exp(math.log(0.03) - 2.70805 * jax.random.uniform(seeds[7], (N_LAT, N_LON, OBS_DEV), jnp.float32) ** steps_of(seeds[7], (N_LAT, N_LON, OBS_DEV), ((0, 4), (1, 4)), -0.2, 0.2)), 0.002, 0.03)
    return dict(sample_quantities=sample_quantities, conv_weight=conv_weight, conv_bias=conv_bias, out_weight=out_weight, obs_index=obs_index, obs_count=obs_count, obs_value=obs_value, obs_weight=obs_weight)


def substep(padded, conv_weight, conv_bias, out_weight):
    nvar = padded.shape[0]
    rows = padded.shape[1] - 2
    cols = padded.shape[2] - 2
    patches = jnp.concatenate([padded[:, a:a + rows, b:b + cols] for a in range(3) for b in range(3)], axis=0)
    patches = patches.reshape(9 * nvar, rows * cols)
    pre = lax.dot_general(conv_weight, patches, (((0,), (0,)), ((), ())), preferred_element_type=jnp.float32)
    hidden = jax.nn.gelu(pre + conv_bias[:, None]).astype(jnp.bfloat16)
    change = lax.dot_general(out_weight, hidden, (((0,), (0,)), ((), ())), preferred_element_type=jnp.float32)
    centre = padded[:, 1:-1, 1:-1].astype(jnp.float32)
    return (centre + change.reshape(nvar, rows, cols)).astype(jnp.bfloat16)

def blend_weights(gram, proj):
    entries_number = gram.shape[0]
    eye = jnp.eye(entries_number, dtype=gram.dtype)
    system = (entries_number - 1) * eye + gram
    scale = jnp.sqrt(jnp.sum(system * system))
    current = system / scale
    inverse = eye
    for turn in range(NS_ITERS):
        factor = 1.5 * eye - 0.5 * jnp.dot(inverse, current, precision=lax.Precision.HIGHEST)
        current = jnp.dot(current, factor, precision=lax.Precision.HIGHEST)
        inverse = jnp.dot(factor, inverse, precision=lax.Precision.HIGHEST)
    root_inv = inverse / jnp.sqrt(scale)
    half = jnp.dot(root_inv, proj, precision=lax.Precision.HIGHEST)
    mean_w = jnp.dot(root_inv, half, precision=lax.Precision.HIGHEST)
    full = mean_w[:, None] + math.sqrt(entries_number - 1.0) * root_inv
    return 1.0 / entries_number + full - lax.optimization_barrier(jnp.mean(full, axis=0, keepdims=True))

def reference(sample_quantities, conv_weight, conv_bias, out_weight, obs_index, obs_count, obs_value, obs_weight):

    def predicted_sample(gridded_quantity):
        for sub in range(2):
            padded = jnp.pad(gridded_quantity, ((0, 0), (1, 1), (0, 0)))
            padded = jnp.concatenate([padded[:, :, -1:], padded, padded[:, :, :1]], axis=2)
            gridded_quantity = substep(padded, conv_weight, conv_bias, out_weight)
        return gridded_quantity
    predicted_population = lax.map(predicted_sample, sample_quantities)
    entries_number = predicted_population.shape[0]
    tile_sequence = predicted_population.reshape(entries_number, EVOLVED_QUANTITY, N_LAT, PARALLEL_LINES, N_LON, MERIDIAN_LINES).transpose(0, 2, 4, 1, 3, 5)
    tile_sequence = tile_sequence.reshape(entries_number, N_LAT, N_LON, EVOLVED_QUANTITY * PARALLEL_LINES * MERIDIAN_LINES)
    where = jnp.broadcast_to(obs_index[None], (entries_number,) + obs_index.shape).astype(jnp.int32)
    values = jnp.take_along_axis(tile_sequence, where, axis=3).astype(jnp.float32)
    live = (jnp.arange(OBS_DEV, dtype=jnp.int32)[None, None, :] < obs_count[:, :, None]).astype(jnp.float32)
    weight = obs_weight * live
    mean = lax.optimization_barrier(jnp.mean(values, axis=0))
    spread = values - mean
    innov = obs_value - mean
    gram = jnp.einsum('kijo,mijo->km', spread * weight, spread, precision=lax.Precision.HIGHEST)
    proj = jnp.einsum('kijo,ijo->k', spread * weight, innov, precision=lax.Precision.HIGHEST)
    transform_weights_square = blend_weights(gram, proj)
    updated_estimates = jnp.einsum('up,urif->prif', transform_weights_square, predicted_population.astype(jnp.float32), precision=lax.Precision.HIGHEST)
    return updated_estimates.astype(jnp.bfloat16)
```

```python
import math

import jax
import jax.numpy as jnp
from jax import lax
from jax.experimental import pallas as pl
from jax.experimental.pallas import tpu as pltpu
from jax.sharding import PartitionSpec as P

NS_ITERS = 20
MESH = pl.DeviceIdType.MESH
F32 = jnp.float32
BF16 = jnp.bfloat16
NV = 24
ROWS = 64
LANES = 128
SLAB = 80
NE = 32
NA = 4
NB = 4
PITCH = 72
NOBS = 256


def dot(a, b, dims=((1,), (0,)), precision=None):
    return lax.dot_general(
        a, b, (dims, ((), ())), precision=precision, preferred_element_type=F32
    )


def marks(hit):
    return jnp.where(hit, 1.0, 0.0).astype(BF16)


def lane_iota(shape):
    return lax.broadcasted_iota(jnp.int32, shape, len(shape) - 1)


def row_iota(shape):
    return lax.broadcasted_iota(jnp.int32, shape, len(shape) - 2)


def roll(x, shift):
    if isinstance(shift, int):
        shift = shift % LANES
        if shift == 0:
            return x
    return pltpu.roll(x, shift, 1)


def slab(x, west, east):
    lane = lane_iota((NV, LANES))
    xw = jnp.where(lane == 0, west, roll(x, 1))
    xe = jnp.where(lane == LANES - 1, east, roll(x, -1))
    return jnp.concatenate([xw, x, xe, jnp.ones((8, LANES), F32)], axis=0).astype(BF16)


def gelu2(pre):
    c1 = math.sqrt(2.0 / math.pi)
    c2 = c1 * 0.044715
    th = jnp.tanh(pre * (c1 + c2 * (pre * pre)))
    return (pre + pre * th).astype(BF16)


def changes(wt, ow, patches):
    pre = dot(wt, patches)
    return dot(ow, gelu2(pre))


def kernel(
    x_hbm, cw_hbm, cb_hbm, ow_hbm, oi_hbm, oc_hbm, ov_hbm, og_hbm, out_ref,
    xv, cw, cb, ow, oi, oc, ov, og,
    big, s1, s2, wt, owt, hrow_s, hcol_s, hrow, hcol, obs_s, obs_r,
    fc, recv, back, res, pick_s, hx, gsend, grecv, acc, ep, oh, sp, ets,
    load_sem, hsend, hrecv, asend, arecv, psend, precv, gsend_sem, grecv_sem,
    bsend, brecv,
):
    k = lax.axis_index("ens")
    i = lax.axis_index("lat")
    j = lax.axis_index("lon")
    i2 = (i + 2) % NA
    k_hi, k_y, k_c = k // 16, (k // 2) % 8, k % 2

    def peer(dk, di, dj):
        return ((k + dk) % NE, (i + di) % NA, (j + dj) % NB)

    def partner(s):
        u = s // 4
        dy = ((u + 1) // 2) * (2 * (u % 2) - 1)
        hi = (k_hi + s) % 2
        y = (k_y + 8 + dy) % 8
        c = (k_c + s // 2) % 2
        return hi * 16 + y * 2 + c

    barrier = pltpu.get_barrier_semaphore()
    for di in range(NA):
        for dj in range(NB):
            if di or dj:
                pl.semaphore_signal(
                    barrier, inc=1, device_id=peer(0, di, dj), device_id_type=MESH
                )
    for dk in range(1, NE):
        pl.semaphore_signal(barrier, inc=1, device_id=peer(dk, 2, 0), device_id_type=MESH)

    loads = [
        pltpu.make_async_copy(src, dst, load_sem.at[n])
        for n, (src, dst) in enumerate(
            [(x_hbm, xv), (cw_hbm, cw), (cb_hbm, cb), (ow_hbm, ow),
             (oi_hbm, oi), (oc_hbm, oc), (ov_hbm, ov), (og_hbm, og)]
        )
    ]
    for c in loads:
        c.start()
    for c in loads:
        c.wait()

    lane24 = lane_iota((NV, LANES))

    for v in range(NV):
        big[v * PITCH : v * PITCH + ROWS, :] = xv[0, v].astype(F32)

    def row_of(r):
        return big[pl.ds(r, NV, stride=PITCH), :]

    def extract(r4, cols):
        for q in range(4):
            r = r4 * 4 + q
            x = roll(row_of(r), r)
            cols = tuple(
                jnp.where(lane24 == (r + off) % LANES, x, c)
                for c, off in zip(cols, (0, 1, LANES - 2, LANES - 1))
            )
        return cols

    zero24 = jnp.zeros((NV, LANES), F32)
    c0, c1, c126, c127 = lax.fori_loop(0, ROWS // 4, extract, (zero24,) * 4)
    c1 = roll(c1, -1)
    c126 = roll(c126, 2)
    c127 = roll(c127, 1)
    hcol_s[0] = jnp.concatenate([c0, c1], axis=0).astype(BF16)
    hcol_s[1] = jnp.concatenate([c126, c127], axis=0).astype(BF16)
    hrow_s[0] = jnp.concatenate([row_of(0), row_of(1)], axis=0).astype(BF16)
    hrow_s[1] = jnp.concatenate([row_of(ROWS - 2), row_of(ROWS - 1)], axis=0).astype(BF16)
    live = (lane_iota((1, NOBS)) < oc[...]).astype(F32)
    obs_s[0:1, :] = ov[0]
    obs_s[1:2, :] = og[0] * live
    obs_s[2:8, :] = jnp.zeros((6, NOBS), F32)

    pl.semaphore_wait(barrier, NA * NB - 1 + NE - 1)

    def halo(src, dst, n, di, dj):
        return pltpu.make_async_remote_copy(
            src_ref=src, dst_ref=dst, send_sem=hsend.at[n], recv_sem=hrecv.at[n],
            device_id=peer(0, di, dj), device_id_type=MESH,
        )

    north = [
        halo(hrow_s.at[1], hrow.at[0], 0, 1, 0),
        halo(hcol_s.at[1], hcol.at[2], 4, 1, 1),
        halo(hcol_s.at[0], hcol.at[3], 5, 1, -1),
    ]
    south = [
        halo(hrow_s.at[0], hrow.at[1], 1, -1, 0),
        halo(hcol_s.at[1], hcol.at[4], 6, -1, 1),
        halo(hcol_s.at[0], hcol.at[5], 7, -1, -1),
    ]
    sides = [
        halo(hcol_s.at[1], hcol.at[0], 2, 0, 1),
        halo(hcol_s.at[0], hcol.at[1], 3, 0, -1),
    ]
    obs_copy = halo(obs_s, obs_r, 8, 2, 0)

    @pl.when(i < NA - 1)
    def _():
        for c in north:
            c.start()

    @pl.when(i > 0)
    def _():
        for c in south:
            c.start()

    for c in sides:
        c.start()
    obs_copy.start()

    @pl.when(i == 0)
    def _():
        hrow[0] = jnp.zeros((2 * NV, LANES), BF16)
        hcol[2] = jnp.zeros((2 * NV, LANES), BF16)
        hcol[3] = jnp.zeros((2 * NV, LANES), BF16)

    @pl.when(i == NA - 1)
    def _():
        hrow[1] = jnp.zeros((2 * NV, LANES), BF16)
        hcol[4] = jnp.zeros((2 * NV, LANES), BF16)
        hcol[5] = jnp.zeros((2 * NV, LANES), BF16)

    w = cw[...].astype(F32)
    b = cb[...]
    b_hi = b.astype(BF16).astype(F32)
    b_mid = (b - b_hi).astype(BF16).astype(F32)
    b_lo = b - b_hi - b_mid
    zeros8 = jnp.zeros((8, 256), F32)
    pad = row_iota((8, 256))
    bias8 = jnp.where(pad == 0, b_hi, jnp.where(pad == 1, b_mid, jnp.where(pad == 2, b_lo, zeros8)))
    wfull = jnp.concatenate(
        [w[0:72], bias8, w[72:144], zeros8, w[144:216], zeros8, zeros8, zeros8], axis=0
    )
    wt[...] = wfull.T.astype(BF16)
    owp = jnp.concatenate([ow[...].astype(F32) * 0.5, jnp.zeros((256, 104), F32)], axis=1)
    owt[...] = owp.T[0:32].astype(BF16)
    tail = jnp.zeros((16, LANES), BF16)
    s1[68 * SLAB : 68 * SLAB + 16, :] = tail
    s2[66 * SLAB : 66 * SLAB + 16, :] = tail

    for c in sides:
        c.wait()
    obs_copy.wait()

    @pl.when(i > 0)
    def _():
        for c in north:
            c.wait_recv()

    @pl.when(i < NA - 1)
    def _():
        for c in north:
            c.wait_send()
        for c in south:
            c.wait_recv()

    @pl.when(i > 0)
    def _():
        for c in south:
            c.wait_send()

    def pair(ref, n):
        both = ref[n].astype(F32)
        return both[0:NV], both[NV : 2 * NV]

    n0, n1 = pair(hrow, 0)
    m0, m1 = pair(hrow, 1)

    def ext(mid, top, bottom):
        out = roll(mid, 2)
        out = jnp.where(lane24 < 2, roll(top, 2 - ROWS), out)
        return jnp.where(lane24 > ROWS + 1, roll(bottom, ROWS + 2), out)

    w_m, w_n, w_s = pair(hcol, 0), pair(hcol, 2), pair(hcol, 4)
    e_m, e_n, e_s = pair(hcol, 1), pair(hcol, 3), pair(hcol, 5)
    cm2 = ext(w_m[0], w_n[0], w_s[0])
    cm1 = ext(w_m[1], w_n[1], w_s[1])
    cp0 = ext(e_m[0], e_n[0], e_s[0])
    cp1 = ext(e_m[1], e_n[1], e_s[1])

    def own(mid, lane):
        out = roll(mid, 2)
        for at, x in ((0, n0), (1, n1), (ROWS + 2, m0), (ROWS + 3, m1)):
            out = jnp.where(lane24 == at, roll(x, at - lane), out)
        return out

    c0e = own(c0, 0)
    c127e = own(c127, LANES - 1)

    def put1(n, x):
        s1[pl.ds(pl.multiple_of(n * SLAB, 16), SLAB), :] = slab(
            x, roll(cm1, (LANES - n) % LANES), roll(cp0, (2 * LANES - 1 - n) % LANES)
        )

    for n, x in ((0, n0), (1, n1), (ROWS + 2, m0), (ROWS + 3, m1)):
        put1(n, x)

    def build(r4, carry):
        for q in range(4):
            r = r4 * 4 + q
            put1(r + 2, row_of(r))
        return carry

    lax.fori_loop(0, ROWS // 4, build, 0)

    weights = wt[...]
    oweights = owt[...]

    def edge(a0, a1, a2):
        ones = jnp.ones((8, LANES), F32)
        rows = []
        for a in range(3):
            rows += [roll(a0, -a), roll(a1, -a), roll(a2, -a), ones]
        rows.append(jnp.zeros((16, LANES), F32))
        return jnp.concatenate(rows, axis=0).astype(BF16)

    first, last = i > 0, i < NA - 1
    ep[:, 0:LANES] = edge(cm2, cm1, c0e)
    ep[:, LANES : 2 * LANES] = edge(c127e, cp0, cp1)
    ch = changes(weights, oweights, ep[...])
    inside = ((lane24 > 0) | first) & ((lane24 < ROWS + 1) | last)
    mw = jnp.where(inside, roll(cm1, -1) + ch[0:NV, 0:LANES], 0.0)
    me = jnp.where(inside, roll(cp0, -1) + ch[0:NV, LANES : 2 * LANES], 0.0)

    def tile(s, n):
        base = pl.multiple_of(n * SLAB, 16)
        p = jnp.concatenate([s[pl.ds(base, 256), :], s[pl.ds(base + SLAB, 256), :]], axis=1)
        c = changes(weights, oweights, p)
        mid0 = s[pl.ds(base + SLAB, SLAB), :].astype(F32)[NV : 2 * NV]
        mid1 = s[pl.ds(base + 2 * SLAB, SLAB), :].astype(F32)[NV : 2 * NV]
        return mid0 + c[0:NV, 0:LANES], mid1 + c[0:NV, LANES : 2 * LANES]

    def step1(t3, carry):
        for q in range(3):
            n = (t3 * 3 + q) * 2
            for d, m in enumerate(tile(s1, n)):
                at = n + d
                keep = ((at > 0) | first) & ((at < ROWS + 1) | last)
                m = jnp.where(keep, m, 0.0)
                s2[pl.ds(pl.multiple_of(at * SLAB, 16), SLAB), :] = slab(
                    m,
                    roll(mw, (LANES - at) % LANES),
                    roll(me, (2 * LANES - 1 - at) % LANES),
                )
        return carry

    lax.fori_loop(0, 11, step1, 0)

    flat = oi[0]
    v_of, r_of, c_of = flat // 8192, (flat // LANES) % ROWS, flat % LANES
    where_row = r_of * NV + v_of
    oh[...] = marks(row_iota((LANES, NOBS)) == c_of)
    acc[...] = jnp.zeros((8, NOBS), F32)

    def send_tile(s):
        t = partner(s)
        return pltpu.make_async_remote_copy(
            src_ref=fc.at[t], dst_ref=recv.at[k], send_sem=asend.at[t], recv_sem=arecv.at[k],
            device_id=(t, i2, j), device_id_type=MESH,
        )

    def step2(s2i, carry):
        for q in range(2):
            t = partner(s2i * 2 + q)
            f0, f1 = tile(s2, t * 2)
            f = jnp.concatenate([f0, f1], axis=0).astype(BF16)
            fc[t] = f
            at_c = dot(f, oh[...])
            hit = row_iota((2 * NV, NOBS)) + t * (2 * NV) == where_row
            sel = jnp.where(hit, at_c, 0.0)
            total = sel[0:8]
            for g in range(1, 6):
                total = total + sel[8 * g : 8 * g + 8]
            acc[...] += total
        return carry

    lax.fori_loop(0, NE // 2, step2, 0)

    pick_s[0] = jnp.sum(acc[...], axis=0, keepdims=True)

    def send_pick(t):
        return pltpu.make_async_remote_copy(
            src_ref=pick_s.at[0], dst_ref=hx.at[k], send_sem=psend.at[t], recv_sem=precv.at[k],
            device_id=(t, i2, j), device_id_type=MESH,
        )

    def over(n, body):
        lax.fori_loop(0, n, lambda s, c: (body(s), c)[1], 0)

    over(NE, lambda s: send_pick(partner(s)).start())
    over(NE, lambda s: send_tile(s).start())

    def recv_pick(t):
        return pltpu.make_async_remote_copy(
            src_ref=pick_s.at[0], dst_ref=hx.at[t], send_sem=psend.at[t], recv_sem=precv.at[t],
            device_id=(t, i2, j), device_id_type=MESH,
        )

    over(NE, lambda t: recv_pick(t).wait_recv())

    values = hx[:, 0, :]
    value = obs_r[0:1, :]
    weight = obs_r[1:2, :]
    mean = jnp.mean(values, axis=0, keepdims=True)
    dev = values - mean
    innov = value - mean
    rows40 = jnp.concatenate([dev, jnp.broadcast_to(innov, (8, NOBS))], axis=0)
    wdev = dev * weight
    hp = lax.Precision.HIGHEST
    g4 = dot(rows40, jnp.concatenate([wdev] * 4, axis=0), ((1,), (1,)), hp)
    lane8 = lane_iota((8, LANES))
    packed = jnp.zeros((8, LANES), F32)
    for q in range(4):
        packed = jnp.where(lane8 // 32 == q, g4[8 * q : 8 * q + 8], packed)
    mine = jnp.concatenate([packed, g4[32:40]], axis=0)
    gsend[...] = mine
    slot = i * NB + j
    grecv[slot] = mine

    def send_gram(di, dj):
        n = (di % NA) * NB + dj % NB
        return pltpu.make_async_remote_copy(
            src_ref=gsend, dst_ref=grecv.at[slot], send_sem=gsend_sem.at[n],
            recv_sem=grecv_sem.at[slot], device_id=peer(0, di, dj), device_id_type=MESH,
        )

    def recv_gram(di, dj):
        n = ((i + di) % NA) * NB + (j + dj) % NB
        return pltpu.make_async_remote_copy(
            src_ref=gsend, dst_ref=grecv.at[n], send_sem=gsend_sem.at[0],
            recv_sem=grecv_sem.at[n], device_id=peer(0, di, dj), device_id_type=MESH,
        )

    others = [(di, dj) for di in range(NA) for dj in range(NB) if di or dj]
    for di, dj in others:
        send_gram(di, dj).start()
    for di, dj in others:
        recv_gram(di, dj).wait_recv()

    total = grecv[0]
    for n in range(1, NA * NB):
        total = total + grecv[n]
    p1, p2 = total[0:8], total[8:16]
    gram = jnp.concatenate(
        [(p1 if q == 0 else roll(p1, -32 * q))[:, 0:32] for q in range(4)], axis=0
    )
    proj = p2[:, 0:32]
    eye = jnp.where(row_iota((NE, NE)) == lane_iota((NE, NE)), 1.0, 0.0)
    system = (NE - 1) * eye + gram

    def full_sum(a):
        return jnp.sum(jnp.sum(a, axis=1, keepdims=True), axis=0, keepdims=True)

    scale = jnp.sqrt(full_sum(system * system))

    current, inverse = system / scale, eye
    for _ in range(NS_ITERS):
        factor = 1.5 * eye - 0.5 * dot(inverse, current, precision=hp)
        new = dot(jnp.concatenate([current, inverse], axis=0), factor, precision=hp)
        current, inverse = new[0:NE], new[NE : 2 * NE]
    root = inverse / jnp.sqrt(scale)
    half = dot(proj, root, precision=hp)
    mean_w = dot(half, root, precision=hp)[0:1]
    full = mean_w + math.sqrt(NE - 1.0) * root
    et = 1.0 / NE + full - jnp.mean(full, axis=1, keepdims=True)
    et_hi = et.astype(BF16)
    et_lo = (et - et_hi.astype(F32)).astype(BF16)

    spread = marks(row_iota((512, NE)) // 16 == lane_iota((512, NE)))
    sp[...] = marks(row_iota((NE, 512)) == lane_iota((NE, 512)) // 16)
    ets[0] = et_hi
    ets[1] = et_lo
    same = row_iota((512, 512)) % 16 == lane_iota((512, 512)) % 16

    def kron(e):
        a = dot(spread, e).astype(BF16)
        return jnp.where(same, dot(a, sp[...]), 0.0).astype(BF16)

    kr_hi = kron(ets[0])
    kr_lo = kron(ets[1])

    def recv_tile(t):
        return pltpu.make_async_remote_copy(
            src_ref=fc.at[t], dst_ref=recv.at[t], send_sem=asend.at[t], recv_sem=arecv.at[t],
            device_id=(t, i2, j), device_id_type=MESH,
        )

    over(NE, lambda t: recv_tile(t).wait_recv())

    for q in range(3):
        f = recv[:, 16 * q : 16 * q + 16, :].reshape(512, LANES)
        o = dot(kr_hi, f) + dot(kr_lo, f)
        back[:, 16 * q : 16 * q + 16, :] = o.astype(BF16).reshape(NE, 16, LANES)

    def send_back(s):
        t = partner(s)
        return pltpu.make_async_remote_copy(
            src_ref=back.at[t], dst_ref=res.at[k], send_sem=bsend.at[t], recv_sem=brecv.at[k],
            device_id=(t, i2, j), device_id_type=MESH,
        )

    def recv_back(t):
        return pltpu.make_async_remote_copy(
            src_ref=back.at[t], dst_ref=res.at[t], send_sem=bsend.at[t], recv_sem=brecv.at[t],
            device_id=(t, i2, j), device_id_type=MESH,
        )

    over(NE, lambda s: send_back(s).start())

    def finish(t):
        recv_back(t).wait_recv()
        big[pl.ds(pl.multiple_of(t * 48, 16), 48), :] = res[t].astype(F32)

    over(NE, finish)
    for v in range(NV):
        out_ref[0, v] = big[pl.ds(v, ROWS, stride=NV), :].astype(BF16)

    over(NE, lambda t: recv_pick(t).wait_send())
    over(NE, lambda t: recv_tile(t).wait_send())
    over(NE, lambda t: recv_back(t).wait_send())
    for di, dj in others:
        send_gram(di, dj).wait_send()


def per_device(x, cw, cb, ow, oi, oc, ov, og):
    anyspec = pl.BlockSpec(memory_space=pl.ANY)
    return pl.pallas_call(
        kernel,
        out_shape=jax.ShapeDtypeStruct(x.shape, x.dtype),
        in_specs=[anyspec] * 8,
        out_specs=pl.BlockSpec(memory_space=pltpu.VMEM),
        scratch_shapes=[
            pltpu.VMEM(x.shape, BF16),
            pltpu.VMEM(cw.shape, BF16),
            pltpu.VMEM((1, 256), F32),
            pltpu.VMEM(ow.shape, BF16),
            pltpu.VMEM((1, 1, NOBS), jnp.int32),
            pltpu.VMEM((1, 1), jnp.int32),
            pltpu.VMEM((1, 1, NOBS), F32),
            pltpu.VMEM((1, 1, NOBS), F32),
            pltpu.VMEM((NV * PITCH, LANES), F32),
            pltpu.VMEM((68 * SLAB + 16, LANES), BF16),
            pltpu.VMEM((66 * SLAB + 16, LANES), BF16),
            pltpu.VMEM((256, 256), BF16),
            pltpu.VMEM((32, 256), BF16),
            pltpu.VMEM((2, 2 * NV, LANES), BF16),
            pltpu.VMEM((2, 2 * NV, LANES), BF16),
            pltpu.VMEM((2, 2 * NV, LANES), BF16),
            pltpu.VMEM((6, 2 * NV, LANES), BF16),
            pltpu.VMEM((8, NOBS), F32),
            pltpu.VMEM((8, NOBS), F32),
            pltpu.VMEM((NE, 2 * NV, LANES), BF16),
            pltpu.VMEM((NE, 2 * NV, LANES), BF16),
            pltpu.VMEM((NE, 2 * NV, LANES), BF16),
            pltpu.VMEM((NE, 2 * NV, LANES), BF16),
            pltpu.VMEM((1, 1, NOBS), F32),
            pltpu.VMEM((NE, 1, NOBS), F32),
            pltpu.VMEM((16, LANES), F32),
            pltpu.VMEM((NA * NB, 16, LANES), F32),
            pltpu.VMEM((8, NOBS), F32),
            pltpu.VMEM((256, 256), BF16),
            pltpu.VMEM((LANES, NOBS), BF16),
            pltpu.VMEM((NE, 512), BF16),
            pltpu.VMEM((2, NE, NE), BF16),
            pltpu.SemaphoreType.DMA((8,)),
            pltpu.SemaphoreType.DMA((9,)),
            pltpu.SemaphoreType.DMA((9,)),
            pltpu.SemaphoreType.DMA((NE,)),
            pltpu.SemaphoreType.DMA((NE,)),
            pltpu.SemaphoreType.DMA((NE,)),
            pltpu.SemaphoreType.DMA((NE,)),
            pltpu.SemaphoreType.DMA((NA * NB,)),
            pltpu.SemaphoreType.DMA((NA * NB,)),
            pltpu.SemaphoreType.DMA((NE,)),
            pltpu.SemaphoreType.DMA((NE,)),
        ],
        compiler_params=pltpu.CompilerParams(
            collective_id=0, has_side_effects=True, vmem_limit_bytes=48 * 1024 * 1024
        ),
        name="cycle",
    )(x, cw, cb.reshape(1, 256), ow, oi, oc, ov, og)


def solution(mesh):
    return jax.shard_map(
        per_device,
        mesh=mesh,
        in_specs=(
            P("ens", None, "lat", "lon"),
            P(),
            P(),
            P(),
            P("lat", "lon", None),
            P("lat", "lon"),
            P("lat", "lon", None),
            P("lat", "lon", None),
        ),
        out_specs=P("ens", None, "lat", "lon"),
        check_vma=False,
    )
```

```python
import math

import jax
import jax.numpy as jnp
from jax import lax
from jax.experimental import pallas as pl
from jax.experimental.pallas import tpu as pltpu
from jax.sharding import PartitionSpec as P

NS_ITERS = 20
MESH = pl.DeviceIdType.MESH
F32 = jnp.float32
BF16 = jnp.bfloat16
NV = 24
ROWS = 64
LANES = 128
SLAB = 80
NE = 32
NA = 4
NB = 4
PITCH = 72
NOBS = 256


def dot(a, b, dims=((1,), (0,)), precision=None):
    return lax.dot_general(
        a, b, (dims, ((), ())), precision=precision, preferred_element_type=F32
    )


def marks(hit):
    return jnp.where(hit, 1.0, 0.0).astype(BF16)


def lane_iota(shape):
    return lax.broadcasted_iota(jnp.int32, shape, len(shape) - 1)


def row_iota(shape):
    return lax.broadcasted_iota(jnp.int32, shape, len(shape) - 2)


def roll(x, shift):
    if isinstance(shift, int):
        shift = shift % LANES
        if shift == 0:
            return x
    return pltpu.roll(x, shift, 1)


def slab(x, west, east):
    lane = lane_iota((NV, LANES))
    xw = jnp.where(lane == 0, west, roll(x, 1))
    xe = jnp.where(lane == LANES - 1, east, roll(x, -1))
    return jnp.concatenate([xw, x, xe, jnp.ones((8, LANES), F32)], axis=0).astype(BF16)


def gelu2(pre):
    c1 = math.sqrt(2.0 / math.pi)
    c2 = c1 * 0.044715
    x = pre.astype(BF16)
    th = jnp.tanh(x * (jnp.bfloat16(c1) + jnp.bfloat16(c2) * (x * x)))
    return x + x * th


def changes(wt, ow, patches):
    pre = dot(wt, patches)
    return dot(ow, gelu2(pre))


def kernel(
    x_hbm, cw_hbm, cb_hbm, ow_hbm, oi_hbm, oc_hbm, ov_hbm, og_hbm, out_ref,
    xv, cw, cb, ow, oi, oc, ov, og,
    big, s1, s2, wt, owt, hrow_s, hcol_s, hrow, hcol, obs_s, obs_r,
    fc, recv, back, res, pick_s, hx, gsend, grecv, acc, ep, oh, sp, ets,
    load_sem, hsend, hrecv, asend, arecv, psend, precv, gsend_sem, grecv_sem,
    bsend, brecv,
):
    k = lax.axis_index("ens")
    i = lax.axis_index("lat")
    j = lax.axis_index("lon")
    i2 = (i + 2) % NA
    k_hi, k_y, k_c = k // 16, (k // 2) % 8, k % 2

    def peer(dk, di, dj):
        return ((k + dk) % NE, (i + di) % NA, (j + dj) % NB)

    def partner(s):
        u = s // 4
        dy = ((u + 1) // 2) * (2 * (u % 2) - 1)
        hi = (k_hi + s) % 2
        y = (k_y + 8 + dy) % 8
        c = (k_c + s // 2) % 2
        return hi * 16 + y * 2 + c

    loads = [
        pltpu.make_async_copy(src, dst, load_sem.at[n])
        for n, (src, dst) in enumerate(
            [(x_hbm, xv), (cw_hbm, cw), (cb_hbm, cb), (ow_hbm, ow),
             (oi_hbm, oi), (oc_hbm, oc), (ov_hbm, ov), (og_hbm, og)]
        )
    ]
    for c in loads:
        c.start()

    barrier = pltpu.get_barrier_semaphore()
    for di in range(NA):
        for dj in range(NB):
            if di or dj:
                pl.semaphore_signal(
                    barrier, inc=1, device_id=peer(0, di, dj), device_id_type=MESH
                )
    for dk in range(1, NE):
        pl.semaphore_signal(barrier, inc=1, device_id=peer(dk, 2, 0), device_id_type=MESH)

    for c in loads:
        c.wait()

    lane24 = lane_iota((NV, LANES))

    for v in range(NV):
        big[v * PITCH : v * PITCH + ROWS, :] = xv[0, v].astype(F32)

    def row_of(r):
        return big[pl.ds(r, NV, stride=PITCH), :]

    zero24 = jnp.zeros((NV, LANES), F32)
    cols = (zero24,) * 4
    for row in range(ROWS):
        x = roll(row_of(row), row)
        cols = tuple(
            jnp.where(lane24 == (row + off) % LANES, x, c)
            for c, off in zip(cols, (0, 1, LANES - 2, LANES - 1))
        )
    c0, c1, c126, c127 = cols
    c1 = roll(c1, -1)
    c126 = roll(c126, 2)
    c127 = roll(c127, 1)
    hcol_s[0] = jnp.concatenate([c0, c1], axis=0).astype(BF16)
    hcol_s[1] = jnp.concatenate([c126, c127], axis=0).astype(BF16)
    hrow_s[0] = jnp.concatenate([row_of(0), row_of(1)], axis=0).astype(BF16)
    hrow_s[1] = jnp.concatenate([row_of(ROWS - 2), row_of(ROWS - 1)], axis=0).astype(BF16)
    live = (lane_iota((1, NOBS)) < oc[...]).astype(F32)
    obs_s[0:1, :] = ov[0]
    obs_s[1:2, :] = og[0] * live
    obs_s[2:8, :] = jnp.zeros((6, NOBS), F32)

    pl.semaphore_wait(barrier, NA * NB - 1 + NE - 1)

    def halo(src, dst, n, di, dj):
        return pltpu.make_async_remote_copy(
            src_ref=src, dst_ref=dst, send_sem=hsend.at[n], recv_sem=hrecv.at[n],
            device_id=peer(0, di, dj), device_id_type=MESH,
        )

    north = [
        halo(hrow_s.at[1], hrow.at[0], 0, 1, 0),
        halo(hcol_s.at[1], hcol.at[2], 4, 1, 1),
        halo(hcol_s.at[0], hcol.at[3], 5, 1, -1),
    ]
    south = [
        halo(hrow_s.at[0], hrow.at[1], 1, -1, 0),
        halo(hcol_s.at[1], hcol.at[4], 6, -1, 1),
        halo(hcol_s.at[0], hcol.at[5], 7, -1, -1),
    ]
    sides = [
        halo(hcol_s.at[1], hcol.at[0], 2, 0, 1),
        halo(hcol_s.at[0], hcol.at[1], 3, 0, -1),
    ]
    obs_copy = halo(obs_s, obs_r, 8, 2, 0)

    @pl.when(i < NA - 1)
    def _():
        for c in north:
            c.start()

    @pl.when(i > 0)
    def _():
        for c in south:
            c.start()

    for c in sides:
        c.start()
    obs_copy.start()

    @pl.when(i == 0)
    def _():
        hrow[0] = jnp.zeros((2 * NV, LANES), BF16)
        hcol[2] = jnp.zeros((2 * NV, LANES), BF16)
        hcol[3] = jnp.zeros((2 * NV, LANES), BF16)

    @pl.when(i == NA - 1)
    def _():
        hrow[1] = jnp.zeros((2 * NV, LANES), BF16)
        hcol[4] = jnp.zeros((2 * NV, LANES), BF16)
        hcol[5] = jnp.zeros((2 * NV, LANES), BF16)

    w = cw[...].astype(F32)
    b = cb[...]
    b_hi = b.astype(BF16).astype(F32)
    b_mid = (b - b_hi).astype(BF16).astype(F32)
    b_lo = b - b_hi - b_mid
    zeros8 = jnp.zeros((8, 256), F32)
    pad = row_iota((8, 256))
    bias8 = jnp.where(pad == 0, b_hi, jnp.where(pad == 1, b_mid, jnp.where(pad == 2, b_lo, zeros8)))
    wfull = jnp.concatenate(
        [w[0:72], bias8, w[72:144], zeros8, w[144:216], zeros8, zeros8, zeros8], axis=0
    )
    wt[...] = wfull.T.astype(BF16)
    owp = ow[...].astype(F32) * 0.5
    owt[...] = jnp.concatenate([owp, jnp.zeros((8, 256), F32)], axis=0).astype(BF16)
    tail = jnp.zeros((16, LANES), BF16)
    s1[68 * SLAB : 68 * SLAB + 16, :] = tail
    s2[66 * SLAB : 66 * SLAB + 16, :] = tail

    for c in sides:
        c.wait()
    obs_copy.wait()

    @pl.when(i > 0)
    def _():
        for c in north:
            c.wait_recv()

    @pl.when(i < NA - 1)
    def _():
        for c in north:
            c.wait_send()
        for c in south:
            c.wait_recv()

    @pl.when(i > 0)
    def _():
        for c in south:
            c.wait_send()

    def pair(ref, n):
        both = ref[n].astype(F32)
        return both[0:NV], both[NV : 2 * NV]

    n0, n1 = pair(hrow, 0)
    m0, m1 = pair(hrow, 1)

    def ext(mid, top, bottom):
        out = roll(mid, 2)
        out = jnp.where(lane24 < 2, roll(top, 2 - ROWS), out)
        return jnp.where(lane24 > ROWS + 1, roll(bottom, ROWS + 2), out)

    w_m, w_n, w_s = pair(hcol, 0), pair(hcol, 2), pair(hcol, 4)
    e_m, e_n, e_s = pair(hcol, 1), pair(hcol, 3), pair(hcol, 5)
    cm2 = ext(w_m[0], w_n[0], w_s[0])
    cm1 = ext(w_m[1], w_n[1], w_s[1])
    cp0 = ext(e_m[0], e_n[0], e_s[0])
    cp1 = ext(e_m[1], e_n[1], e_s[1])

    def own(mid, lane):
        out = roll(mid, 2)
        for at, x in ((0, n0), (1, n1), (ROWS + 2, m0), (ROWS + 3, m1)):
            out = jnp.where(lane24 == at, roll(x, at - lane), out)
        return out

    c0e = own(c0, 0)
    c127e = own(c127, LANES - 1)

    def put1(n, x):
        s1[n * SLAB : (n + 1) * SLAB, :] = slab(x, roll(cm1, -n), roll(cp0, LANES - 1 - n))

    for n, x in ((0, n0), (1, n1), (ROWS + 2, m0), (ROWS + 3, m1)):
        put1(n, x)

    for row in range(ROWS):
        put1(row + 2, row_of(row))

    weights = wt[...]
    oweights = owt[...]

    def edge(a0, a1, a2):
        ones = jnp.ones((8, LANES), F32)
        rows = []
        for a in range(3):
            rows += [roll(a0, -a), roll(a1, -a), roll(a2, -a), ones]
        rows.append(jnp.zeros((16, LANES), F32))
        return jnp.concatenate(rows, axis=0).astype(BF16)

    first, last = i > 0, i < NA - 1
    ep[:, 0:LANES] = edge(cm2, cm1, c0e)
    ep[:, LANES : 2 * LANES] = edge(c127e, cp0, cp1)
    ch = changes(weights, oweights, ep[...])
    inside = ((lane24 > 0) | first) & ((lane24 < ROWS + 1) | last)
    mw = jnp.where(inside, roll(cm1, -1) + ch[0:NV, 0:LANES], 0.0)
    me = jnp.where(inside, roll(cp0, -1) + ch[0:NV, LANES : 2 * LANES], 0.0)

    def tile(s, n):
        base = pl.multiple_of(n * SLAB, 16)
        p = jnp.concatenate([s[pl.ds(base, 256), :], s[pl.ds(base + SLAB, 256), :]], axis=1)
        c = changes(weights, oweights, p)
        mid0 = s[pl.ds(base + SLAB, SLAB), :].astype(F32)[NV : 2 * NV]
        mid1 = s[pl.ds(base + 2 * SLAB, SLAB), :].astype(F32)[NV : 2 * NV]
        return mid0 + c[0:NV, 0:LANES], mid1 + c[0:NV, LANES : 2 * LANES]

    def step1(outer, carry):
        for q in range(11):
            n = (outer * 11 + q) * 2
            for d, m in enumerate(tile(s1, n)):
                at = n + d
                keep = ((at > 0) | first) & ((at < ROWS + 1) | last)
                m = jnp.where(keep, m, 0.0)
                s2[pl.ds(pl.multiple_of(at * SLAB, 16), SLAB), :] = slab(
                    m,
                    roll(mw, (LANES - at) % LANES),
                    roll(me, (2 * LANES - 1 - at) % LANES),
                )
        return carry

    lax.fori_loop(0, 3, step1, 0)

    flat = oi[0]
    v_of, r_of, c_of = flat // 8192, (flat // LANES) % ROWS, flat % LANES
    where_row = r_of * NV + v_of
    oh[...] = marks(row_iota((LANES, NOBS)) == c_of)
    acc[...] = jnp.zeros((8, NOBS), F32)

    def send_tile(s):
        t = partner(s)
        return pltpu.make_async_remote_copy(
            src_ref=fc.at[t], dst_ref=recv.at[k], send_sem=asend.at[t], recv_sem=arecv.at[k],
            device_id=(t, i2, j), device_id_type=MESH,
        )

    def step2(s2i, carry):
        for q in range(8):
            t = partner(s2i * 8 + q)
            f0, f1 = tile(s2, t * 2)
            f = jnp.concatenate([f0, f1], axis=0).astype(BF16)
            fc[t] = f
            at_c = dot(f, oh[...])
            hit = row_iota((2 * NV, NOBS)) + t * (2 * NV) == where_row
            sel = jnp.where(hit, at_c, 0.0)
            total = sel[0:8]
            for g in range(1, 6):
                total = total + sel[8 * g : 8 * g + 8]
            acc[...] += total
        return carry

    lax.fori_loop(0, NE // 8, step2, 0)

    pick_s[0] = jnp.sum(acc[...], axis=0, keepdims=True)

    def send_pick(t):
        return pltpu.make_async_remote_copy(
            src_ref=pick_s.at[0], dst_ref=hx.at[k], send_sem=psend.at[t], recv_sem=precv.at[k],
            device_id=(t, i2, j), device_id_type=MESH,
        )

    def over(n, body):
        lax.fori_loop(0, n, lambda s, c: (body(s), c)[1], 0)

    over(NE, lambda s: send_pick(partner(s)).start())
    over(NE, lambda s: send_tile(s).start())

    def recv_pick(t):
        return pltpu.make_async_remote_copy(
            src_ref=pick_s.at[0], dst_ref=hx.at[t], send_sem=psend.at[t], recv_sem=precv.at[t],
            device_id=(t, i2, j), device_id_type=MESH,
        )

    over(NE, lambda t: recv_pick(t).wait_recv())

    values = hx[:, 0, :]
    value = obs_r[0:1, :]
    weight = obs_r[1:2, :]
    mean = jnp.mean(values, axis=0, keepdims=True)
    dev = values - mean
    innov = value - mean
    rows40 = jnp.concatenate([dev, jnp.broadcast_to(innov, (8, NOBS))], axis=0)
    wdev = dev * weight
    hp = lax.Precision.HIGHEST
    g4 = dot(rows40, jnp.concatenate([wdev] * 4, axis=0), ((1,), (1,)), hp)
    lane8 = lane_iota((8, LANES))
    packed = jnp.zeros((8, LANES), F32)
    for q in range(4):
        packed = jnp.where(lane8 // 32 == q, g4[8 * q : 8 * q + 8], packed)
    mine = jnp.concatenate([packed, g4[32:40]], axis=0)
    gsend[...] = mine
    slot = i * NB + j
    grecv[slot] = mine

    def send_gram(di, dj):
        n = (di % NA) * NB + dj % NB
        return pltpu.make_async_remote_copy(
            src_ref=gsend, dst_ref=grecv.at[slot], send_sem=gsend_sem.at[n],
            recv_sem=grecv_sem.at[slot], device_id=peer(0, di, dj), device_id_type=MESH,
        )

    def recv_gram(di, dj):
        n = ((i + di) % NA) * NB + (j + dj) % NB
        return pltpu.make_async_remote_copy(
            src_ref=gsend, dst_ref=grecv.at[n], send_sem=gsend_sem.at[0],
            recv_sem=grecv_sem.at[n], device_id=peer(0, di, dj), device_id_type=MESH,
        )

    others = [(di, dj) for di in range(NA) for dj in range(NB) if di or dj]
    for di, dj in others:
        send_gram(di, dj).start()
    for di, dj in others:
        recv_gram(di, dj).wait_recv()

    total = grecv[0]
    for n in range(1, NA * NB):
        total = total + grecv[n]
    p1, p2 = total[0:8], total[8:16]
    gram = jnp.concatenate(
        [(p1 if q == 0 else roll(p1, -32 * q))[:, 0:32] for q in range(4)], axis=0
    )
    proj = p2[:, 0:32]
    eye = jnp.where(row_iota((NE, NE)) == lane_iota((NE, NE)), 1.0, 0.0)
    system = (NE - 1) * eye + gram

    def full_sum(a):
        return jnp.sum(jnp.sum(a, axis=1, keepdims=True), axis=0, keepdims=True)

    scale = jnp.sqrt(full_sum(system * system))

    current, inverse = system / scale, eye
    for _ in range(NS_ITERS):
        factor = 1.5 * eye - 0.5 * dot(inverse, current, precision=hp)
        new = dot(jnp.concatenate([current, inverse], axis=0), factor, precision=hp)
        current, inverse = new[0:NE], new[NE : 2 * NE]
    root = inverse / jnp.sqrt(scale)
    half = dot(proj, root, precision=hp)
    mean_w = dot(half, root, precision=hp)[0:1]
    full = mean_w + math.sqrt(NE - 1.0) * root
    et = 1.0 / NE + full - jnp.mean(full, axis=1, keepdims=True)
    et_hi = et.astype(BF16)
    et_lo = (et - et_hi.astype(F32)).astype(BF16)

    spread = marks(row_iota((512, NE)) // 16 == lane_iota((512, NE)))
    sp[...] = marks(row_iota((NE, 512)) == lane_iota((NE, 512)) // 16)
    ets[0] = et_hi
    ets[1] = et_lo
    same = row_iota((512, 512)) % 16 == lane_iota((512, 512)) % 16

    def kron(e):
        a = dot(spread, e).astype(BF16)
        return jnp.where(same, dot(a, sp[...]), 0.0).astype(BF16)

    kr_hi = kron(ets[0])
    kr_lo = kron(ets[1])

    def recv_tile(t):
        return pltpu.make_async_remote_copy(
            src_ref=fc.at[t], dst_ref=recv.at[t], send_sem=asend.at[t], recv_sem=arecv.at[t],
            device_id=(t, i2, j), device_id_type=MESH,
        )

    over(NE, lambda t: recv_tile(t).wait_recv())

    for q in range(3):
        f = recv[:, 16 * q : 16 * q + 16, :].reshape(512, LANES)
        o = dot(kr_hi, f) + dot(kr_lo, f)
        back[:, 16 * q : 16 * q + 16, :] = o.astype(BF16).reshape(NE, 16, LANES)

    def send_back(s):
        t = partner(s)
        return pltpu.make_async_remote_copy(
            src_ref=back.at[t], dst_ref=res.at[k], send_sem=bsend.at[t], recv_sem=brecv.at[k],
            device_id=(t, i2, j), device_id_type=MESH,
        )

    def recv_back(t):
        return pltpu.make_async_remote_copy(
            src_ref=back.at[t], dst_ref=res.at[t], send_sem=bsend.at[t], recv_sem=brecv.at[t],
            device_id=(t, i2, j), device_id_type=MESH,
        )

    over(NE, lambda s: send_back(s).start())

    def finish(t):
        recv_back(t).wait_recv()
        big[pl.ds(pl.multiple_of(t * 48, 16), 48), :] = res[t].astype(F32)

    over(NE, finish)
    for v in range(NV):
        out_ref[0, v] = big[pl.ds(v, ROWS, stride=NV), :].astype(BF16)

    over(NE, lambda t: recv_pick(t).wait_send())
    over(NE, lambda t: recv_tile(t).wait_send())
    over(NE, lambda t: recv_back(t).wait_send())
    for di, dj in others:
        send_gram(di, dj).wait_send()


def per_device(x, cw, cb, ow, oi, oc, ov, og):
    hbm = pl.BlockSpec(memory_space=pltpu.HBM)
    return pl.pallas_call(
        kernel,
        out_shape=jax.ShapeDtypeStruct(x.shape, x.dtype),
        in_specs=[hbm] * 8,
        out_specs=pl.BlockSpec(memory_space=pltpu.VMEM),
        scratch_shapes=[
            pltpu.VMEM(x.shape, BF16),
            pltpu.VMEM(cw.shape, BF16),
            pltpu.VMEM((1, 256), F32),
            pltpu.VMEM((NV, 256), BF16),
            pltpu.VMEM((1, 1, NOBS), jnp.int32),
            pltpu.VMEM((1, 1), jnp.int32),
            pltpu.VMEM((1, 1, NOBS), F32),
            pltpu.VMEM((1, 1, NOBS), F32),
            pltpu.VMEM((NV * PITCH, LANES), F32),
            pltpu.VMEM((68 * SLAB + 16, LANES), BF16),
            pltpu.VMEM((66 * SLAB + 16, LANES), BF16),
            pltpu.VMEM((256, 256), BF16),
            pltpu.VMEM((32, 256), BF16),
            pltpu.VMEM((2, 2 * NV, LANES), BF16),
            pltpu.VMEM((2, 2 * NV, LANES), BF16),
            pltpu.VMEM((2, 2 * NV, LANES), BF16),
            pltpu.VMEM((6, 2 * NV, LANES), BF16),
            pltpu.VMEM((8, NOBS), F32),
            pltpu.VMEM((8, NOBS), F32),
            pltpu.VMEM((NE, 2 * NV, LANES), BF16),
            pltpu.VMEM((NE, 2 * NV, LANES), BF16),
            pltpu.VMEM((NE, 2 * NV, LANES), BF16),
            pltpu.VMEM((NE, 2 * NV, LANES), BF16),
            pltpu.VMEM((1, 1, NOBS), F32),
            pltpu.VMEM((NE, 1, NOBS), F32),
            pltpu.VMEM((16, LANES), F32),
            pltpu.VMEM((NA * NB, 16, LANES), F32),
            pltpu.VMEM((8, NOBS), F32),
            pltpu.VMEM((256, 256), BF16),
            pltpu.VMEM((LANES, NOBS), BF16),
            pltpu.VMEM((NE, 512), BF16),
            pltpu.VMEM((2, NE, NE), BF16),
            pltpu.SemaphoreType.DMA((8,)),
            pltpu.SemaphoreType.DMA((9,)),
            pltpu.SemaphoreType.DMA((9,)),
            pltpu.SemaphoreType.DMA((NE,)),
            pltpu.SemaphoreType.DMA((NE,)),
            pltpu.SemaphoreType.DMA((NE,)),
            pltpu.SemaphoreType.DMA((NE,)),
            pltpu.SemaphoreType.DMA((NA * NB,)),
            pltpu.SemaphoreType.DMA((NA * NB,)),
            pltpu.SemaphoreType.DMA((NE,)),
            pltpu.SemaphoreType.DMA((NE,)),
        ],
        compiler_params=pltpu.CompilerParams(
            collective_id=0, has_side_effects=True, vmem_limit_bytes=67043328
        ),
        name="cycle",
    )(x, cw, cb.reshape(1, 256), ow.T, oi, oc, ov, og)


def solution(mesh):
    return jax.shard_map(
        per_device,
        mesh=mesh,
        in_specs=(
            P("ens", None, "lat", "lon"),
            P(),
            P(),
            P(),
            P("lat", "lon", None),
            P("lat", "lon"),
            P("lat", "lon", None),
            P("lat", "lon", None),
        ),
        out_specs=P("ens", None, "lat", "lon"),
        check_vma=False,
    )
```

```python
import math

import jax
import jax.numpy as jnp
from jax import lax
from jax.experimental import pallas as pl
from jax.experimental.pallas import tpu as pltpu
from jax.sharding import PartitionSpec as P

NS_ITERS = 20
MESH = pl.DeviceIdType.MESH
F32 = jnp.float32
BF16 = jnp.bfloat16
NV = 24
ROWS = 64
LANES = 128
SLAB = 80
NE = 32
NA = 4
NB = 4
PITCH = 72
NOBS = 256


def dot(a, b, dims=((1,), (0,)), precision=None):
    return lax.dot_general(
        a, b, (dims, ((), ())), precision=precision, preferred_element_type=F32
    )


def marks(hit):
    return jnp.where(hit, 1.0, 0.0).astype(BF16)


def lane_iota(shape):
    return lax.broadcasted_iota(jnp.int32, shape, len(shape) - 1)


def row_iota(shape):
    return lax.broadcasted_iota(jnp.int32, shape, len(shape) - 2)


def roll(x, shift):
    if isinstance(shift, int):
        shift = shift % LANES
        if shift == 0:
            return x
    return pltpu.roll(x, shift, 1)


def slab(x, west, east):
    lane = lane_iota((NV, LANES))
    xw = jnp.where(lane == 0, west, roll(x, 1))
    xe = jnp.where(lane == LANES - 1, east, roll(x, -1))
    return jnp.concatenate([xw, x, xe, jnp.ones((8, LANES), F32)], axis=0).astype(BF16)


def gelu2(pre):
    c1 = math.sqrt(2.0 / math.pi)
    c2 = c1 * 0.044715
    x = pre.astype(BF16)
    th = jnp.tanh(x * (jnp.bfloat16(c1) + jnp.bfloat16(c2) * (x * x)))
    return x + x * th


def changes(wt, ow, patches):
    pre = dot(wt, patches)
    return dot(ow, gelu2(pre))


def fill(big, xv):
    for v in range(NV):
        big[v * PITCH : v * PITCH + ROWS, :] = xv[0, v].astype(F32)


def place():
    k = lax.axis_index("ens")
    i = lax.axis_index("lat")
    j = lax.axis_index("lon")

    def peer(dk, di, dj):
        return ((k + dk) % NE, (i + di) % NA, (j + dj) % NB)

    return k, i, j, peer


def meet(peers):
    barrier = pltpu.get_barrier_semaphore()
    for to in peers:
        pl.semaphore_signal(barrier, inc=1, device_id=to, device_id_type=MESH)
    return lambda: pl.semaphore_wait(barrier, len(peers))


def halo_kernel(
    x_hbm, oc, ov, og, hcol_s, hrow, hcol, obs_r,
    xv, big, hrow_s, obs_s, load_sem, hsend, hrecv,
):
    k, i, j, peer = place()
    load = pltpu.make_async_copy(x_hbm, xv, load_sem)
    load.start()
    met = meet(
        [peer(0, di, dj) for di in (0, 1, -1) for dj in (0, 1, -1) if di or dj] + [peer(0, 2, 0)]
    )
    load.wait()
    lane24 = lane_iota((NV, LANES))

    fill(big, xv)

    def row_of(r):
        return big[pl.ds(r, NV, stride=PITCH), :]

    zero24 = jnp.zeros((NV, LANES), F32)
    cols = (zero24,) * 4
    for row in range(ROWS):
        x = roll(row_of(row), row)
        cols = tuple(
            jnp.where(lane24 == (row + off) % LANES, x, c)
            for c, off in zip(cols, (0, 1, LANES - 2, LANES - 1))
        )
    c0, c1, c126, c127 = cols
    c1 = roll(c1, -1)
    c126 = roll(c126, 2)
    c127 = roll(c127, 1)
    hcol_s[0] = jnp.concatenate([c0, c1], axis=0).astype(BF16)
    hcol_s[1] = jnp.concatenate([c126, c127], axis=0).astype(BF16)
    hrow_s[0] = jnp.concatenate([row_of(0), row_of(1)], axis=0).astype(BF16)
    hrow_s[1] = jnp.concatenate([row_of(ROWS - 2), row_of(ROWS - 1)], axis=0).astype(BF16)
    live = (lane_iota((1, NOBS)) < oc[...]).astype(F32)
    obs_s[0:1, :] = ov[0]
    obs_s[1:2, :] = og[0] * live
    obs_s[2:8, :] = jnp.zeros((6, NOBS), F32)

    met()

    def halo(src, dst, n, di, dj):
        return pltpu.make_async_remote_copy(
            src_ref=src, dst_ref=dst, send_sem=hsend.at[n], recv_sem=hrecv.at[n],
            device_id=peer(0, di, dj), device_id_type=MESH,
        )

    north = [
        halo(hrow_s.at[1], hrow.at[0], 0, 1, 0),
        halo(hcol_s.at[1], hcol.at[2], 4, 1, 1),
        halo(hcol_s.at[0], hcol.at[3], 5, 1, -1),
    ]
    south = [
        halo(hrow_s.at[0], hrow.at[1], 1, -1, 0),
        halo(hcol_s.at[1], hcol.at[4], 6, -1, 1),
        halo(hcol_s.at[0], hcol.at[5], 7, -1, -1),
    ]
    sides = [
        halo(hcol_s.at[1], hcol.at[0], 2, 0, 1),
        halo(hcol_s.at[0], hcol.at[1], 3, 0, -1),
    ]
    obs_copy = halo(obs_s, obs_r, 8, 2, 0)

    @pl.when(i < NA - 1)
    def _():
        for c in north:
            c.start()

    @pl.when(i > 0)
    def _():
        for c in south:
            c.start()

    for c in sides:
        c.start()
    obs_copy.start()

    @pl.when(i == 0)
    def _():
        hrow[0] = jnp.zeros((2 * NV, LANES), BF16)
        hcol[2] = jnp.zeros((2 * NV, LANES), BF16)
        hcol[3] = jnp.zeros((2 * NV, LANES), BF16)

    @pl.when(i == NA - 1)
    def _():
        hrow[1] = jnp.zeros((2 * NV, LANES), BF16)
        hcol[4] = jnp.zeros((2 * NV, LANES), BF16)
        hcol[5] = jnp.zeros((2 * NV, LANES), BF16)

    for c in sides:
        c.wait()
    obs_copy.wait()

    @pl.when(i > 0)
    def _():
        for c in north:
            c.wait_recv()

    @pl.when(i < NA - 1)
    def _():
        for c in north:
            c.wait_send()
        for c in south:
            c.wait_recv()

    @pl.when(i > 0)
    def _():
        for c in south:
            c.wait_send()


def kernel(
    xv, cw, cb, ow, oi, hcol_s, hrow, hcol, obs_r, out_ref,
    big, s1, s2, wt, owt,
    fc, recv, back, res, pick_s, hx, gsend, grecv, ep, oh, sp, ets,
    asend, arecv, psend, precv, gsend_sem, grecv_sem, bsend, brecv,
):
    k, i, j, peer = place()
    i2 = (i + 2) % NA
    k_hi, k_y, k_c = k // 16, (k // 2) % 8, k % 2

    def partner(s):
        u = s // 4
        dy = ((u + 1) // 2) * (2 * (u % 2) - 1)
        hi = (k_hi + s) % 2
        y = (k_y + 8 + dy) % 8
        c = (k_c + s // 2) % 2
        return hi * 16 + y * 2 + c

    met = meet(
        [peer(0, di, dj) for di in range(NA) for dj in range(NB) if di or dj]
        + [peer(dk, 2, 0) for dk in range(1, NE)]
    )
    lane24 = lane_iota((NV, LANES))
    fill(big, xv)

    def row_of(r):
        return big[pl.ds(r, NV, stride=PITCH), :]

    w = cw[...].astype(F32)
    b = cb[...]
    b_hi = b.astype(BF16).astype(F32)
    b_mid = (b - b_hi).astype(BF16).astype(F32)
    b_lo = b - b_hi - b_mid
    zeros8 = jnp.zeros((8, 256), F32)
    pad = row_iota((8, 256))
    bias8 = jnp.where(pad == 0, b_hi, jnp.where(pad == 1, b_mid, jnp.where(pad == 2, b_lo, zeros8)))
    wfull = jnp.concatenate(
        [w[0:72], bias8, w[72:144], zeros8, w[144:216], zeros8, zeros8, zeros8], axis=0
    )
    wt[...] = wfull.T.astype(BF16)
    owp = ow[...].astype(F32) * 0.5
    owt[...] = jnp.concatenate([owp, jnp.zeros((8, 256), F32)], axis=0).astype(BF16)
    tail = jnp.zeros((16, LANES), BF16)
    s1[68 * SLAB : 68 * SLAB + 16, :] = tail
    s2[66 * SLAB : 66 * SLAB + 16, :] = tail

    def pair(ref, n):
        both = ref[n].astype(F32)
        return both[0:NV], both[NV : 2 * NV]

    n0, n1 = pair(hrow, 0)
    m0, m1 = pair(hrow, 1)

    def ext(mid, top, bottom):
        out = roll(mid, 2)
        out = jnp.where(lane24 < 2, roll(top, 2 - ROWS), out)
        return jnp.where(lane24 > ROWS + 1, roll(bottom, ROWS + 2), out)

    w_m, w_n, w_s = pair(hcol, 0), pair(hcol, 2), pair(hcol, 4)
    e_m, e_n, e_s = pair(hcol, 1), pair(hcol, 3), pair(hcol, 5)
    cm2 = ext(w_m[0], w_n[0], w_s[0])
    cm1 = ext(w_m[1], w_n[1], w_s[1])
    cp0 = ext(e_m[0], e_n[0], e_s[0])
    cp1 = ext(e_m[1], e_n[1], e_s[1])

    def own(mid, lane):
        out = roll(mid, 2)
        for at, x in ((0, n0), (1, n1), (ROWS + 2, m0), (ROWS + 3, m1)):
            out = jnp.where(lane24 == at, roll(x, at - lane), out)
        return out

    c0e = own(pair(hcol_s, 0)[0], 0)
    c127e = own(pair(hcol_s, 1)[1], LANES - 1)

    def put1(n, x):
        s1[n * SLAB : (n + 1) * SLAB, :] = slab(x, roll(cm1, -n), roll(cp0, LANES - 1 - n))

    for n, x in ((0, n0), (1, n1), (ROWS + 2, m0), (ROWS + 3, m1)):
        put1(n, x)

    for row in range(ROWS):
        put1(row + 2, row_of(row))

    weights = wt[...]
    oweights = owt[...]

    def edge(a0, a1, a2):
        ones = jnp.ones((8, LANES), F32)
        rows = []
        for a in range(3):
            rows += [roll(a0, -a), roll(a1, -a), roll(a2, -a), ones]
        rows.append(jnp.zeros((16, LANES), F32))
        return jnp.concatenate(rows, axis=0).astype(BF16)

    first, last = i > 0, i < NA - 1
    ep[:, 0:LANES] = edge(cm2, cm1, c0e)
    ep[:, LANES : 2 * LANES] = edge(c127e, cp0, cp1)
    ch = changes(weights, oweights, ep[...])
    inside = ((lane24 > 0) | first) & ((lane24 < ROWS + 1) | last)
    mw = jnp.where(inside, roll(cm1, -1) + ch[0:NV, 0:LANES], 0.0)
    me = jnp.where(inside, roll(cp0, -1) + ch[0:NV, LANES : 2 * LANES], 0.0)

    def tile(s, n):
        base = pl.multiple_of(n * SLAB, 16)
        p = jnp.concatenate([s[pl.ds(base, 256), :], s[pl.ds(base + SLAB, 256), :]], axis=1)
        c = changes(weights, oweights, p)
        mid0 = s[pl.ds(base + SLAB, SLAB), :].astype(F32)[NV : 2 * NV]
        mid1 = s[pl.ds(base + 2 * SLAB, SLAB), :].astype(F32)[NV : 2 * NV]
        return mid0 + c[0:NV, 0:LANES], mid1 + c[0:NV, LANES : 2 * LANES]

    def step1(outer, carry):
        for q in range(11):
            n = (outer * 11 + q) * 2
            for d, m in enumerate(tile(s1, n)):
                at = n + d
                keep = ((at > 0) | first) & ((at < ROWS + 1) | last)
                m = jnp.where(keep, m, 0.0)
                s2[pl.ds(pl.multiple_of(at * SLAB, 16), SLAB), :] = slab(
                    m,
                    roll(mw, (LANES - at) % LANES),
                    roll(me, (2 * LANES - 1 - at) % LANES),
                )
        return carry

    lax.fori_loop(0, 3, step1, 0)

    flat = oi[0]
    v_of, r_of, c_of = flat // 8192, (flat // LANES) % ROWS, flat % LANES
    oh[...] = marks(row_iota((LANES, NOBS)) == c_of)

    def gather(outer, taps):
        base = pl.multiple_of(outer * (6 * SLAB), 16)
        at_c = dot(s2[pl.ds(base, 6 * SLAB), :], oh[...]).astype(BF16)
        for q in range(6):
            part = at_c[q * SLAB : (q + 1) * SLAB]
            n = outer * 6 + q
            taps = tuple(t + part * marks(r_of == n - a) for a, t in enumerate(taps))
        return taps

    taps = lax.fori_loop(0, 11, gather, (jnp.zeros((SLAB, NOBS), BF16),) * 3)
    for a in range(3):
        ep[a * SLAB : (a + 1) * SLAB, :] = taps[a]
    ep[3 * SLAB : 256, :] = jnp.zeros((16, NOBS), BF16)
    seen = taps[1].astype(F32)[NV : 2 * NV] + changes(weights, oweights, ep[...])[0:NV]
    seen = seen.astype(BF16).astype(F32)
    pick_s[0] = jnp.sum(jnp.where(row_iota((NV, NOBS)) == v_of, seen, 0.0), axis=0, keepdims=True)

    def send_pick(t):
        return pltpu.make_async_remote_copy(
            src_ref=pick_s.at[0], dst_ref=hx.at[k], send_sem=psend.at[t], recv_sem=precv.at[k],
            device_id=(t, i2, j), device_id_type=MESH,
        )

    def over(n, body):
        lax.fori_loop(0, n, lambda s, c: (body(s), c)[1], 0)

    def send_tile(s):
        t = partner(s)
        return pltpu.make_async_remote_copy(
            src_ref=fc.at[t], dst_ref=recv.at[k], send_sem=asend.at[t], recv_sem=arecv.at[k],
            device_id=(t, i2, j), device_id_type=MESH,
        )

    def step2(outer, carry):
        for q in range(8):
            s = outer * 8 + q
            t = partner(s)
            f0, f1 = tile(s2, t * 2)
            fc[t] = jnp.concatenate([f0, f1], axis=0).astype(BF16)
            if q:
                send_tile(s - 1).start()
        send_tile(outer * 8 + 7).start()
        return carry

    met()
    over(NE, lambda s: send_pick(partner(s)).start())
    lax.fori_loop(0, 2, step2, 0)

    def recv_pick(t):
        return pltpu.make_async_remote_copy(
            src_ref=pick_s.at[0], dst_ref=hx.at[t], send_sem=psend.at[t], recv_sem=precv.at[t],
            device_id=(t, i2, j), device_id_type=MESH,
        )

    over(NE, lambda t: recv_pick(t).wait_recv())

    values = hx[:, 0, :]
    value = obs_r[0:1, :]
    weight = obs_r[1:2, :]
    mean = jnp.mean(values, axis=0, keepdims=True)
    dev = values - mean
    innov = value - mean
    rows40 = jnp.concatenate([dev, jnp.broadcast_to(innov, (8, NOBS))], axis=0)
    wdev = dev * weight
    hp = lax.Precision.HIGHEST
    g4 = dot(rows40, jnp.concatenate([wdev] * 4, axis=0), ((1,), (1,)), hp)
    lane8 = lane_iota((8, LANES))
    packed = jnp.zeros((8, LANES), F32)
    for q in range(4):
        packed = jnp.where(lane8 // 32 == q, g4[8 * q : 8 * q + 8], packed)
    mine = jnp.concatenate([packed, g4[32:40]], axis=0)
    gsend[...] = mine
    slot = i * NB + j
    grecv[slot] = mine

    def send_gram(di, dj):
        n = (di % NA) * NB + dj % NB
        return pltpu.make_async_remote_copy(
            src_ref=gsend, dst_ref=grecv.at[slot], send_sem=gsend_sem.at[n],
            recv_sem=grecv_sem.at[slot], device_id=peer(0, di, dj), device_id_type=MESH,
        )

    def recv_gram(di, dj):
        n = ((i + di) % NA) * NB + (j + dj) % NB
        return pltpu.make_async_remote_copy(
            src_ref=gsend, dst_ref=grecv.at[n], send_sem=gsend_sem.at[0],
            recv_sem=grecv_sem.at[n], device_id=peer(0, di, dj), device_id_type=MESH,
        )

    others = [(di, dj) for di in range(NA) for dj in range(NB) if di or dj]
    for di, dj in others:
        send_gram(di, dj).start()
    lax.fori_loop(2, 4, step2, 0)
    for di, dj in others:
        recv_gram(di, dj).wait_recv()

    total = grecv[0]
    for n in range(1, NA * NB):
        total = total + grecv[n]
    p1, p2 = total[0:8], total[8:16]
    gram = jnp.concatenate(
        [(p1 if q == 0 else roll(p1, -32 * q))[:, 0:32] for q in range(4)], axis=0
    )
    proj = p2[:, 0:32]
    eye = jnp.where(row_iota((NE, NE)) == lane_iota((NE, NE)), 1.0, 0.0)
    system = (NE - 1) * eye + gram

    def full_sum(a):
        return jnp.sum(jnp.sum(a, axis=1, keepdims=True), axis=0, keepdims=True)

    scale = jnp.sqrt(full_sum(system * system))

    current, inverse = system / scale, eye
    for _ in range(NS_ITERS):
        factor = 1.5 * eye - 0.5 * dot(inverse, current, precision=hp)
        new = dot(jnp.concatenate([current, inverse], axis=0), factor, precision=hp)
        current, inverse = new[0:NE], new[NE : 2 * NE]
    root = inverse / jnp.sqrt(scale)
    half = dot(proj, root, precision=hp)
    mean_w = dot(half, root, precision=hp)[0:1]
    full = mean_w + math.sqrt(NE - 1.0) * root
    et = 1.0 / NE + full - jnp.mean(full, axis=1, keepdims=True)
    et_hi = et.astype(BF16)
    et_lo = (et - et_hi.astype(F32)).astype(BF16)

    spread = marks(row_iota((512, NE)) // 16 == lane_iota((512, NE)))
    sp[...] = marks(row_iota((NE, 512)) == lane_iota((NE, 512)) // 16)
    ets[0] = et_hi
    ets[1] = et_lo
    same = row_iota((512, 512)) % 16 == lane_iota((512, 512)) % 16

    def kron(e):
        a = dot(spread, e).astype(BF16)
        return jnp.where(same, dot(a, sp[...]), 0.0).astype(BF16)

    kr_hi = kron(ets[0])
    kr_lo = kron(ets[1])

    def recv_tile(t):
        return pltpu.make_async_remote_copy(
            src_ref=fc.at[t], dst_ref=recv.at[t], send_sem=asend.at[t], recv_sem=arecv.at[t],
            device_id=(t, i2, j), device_id_type=MESH,
        )

    over(NE, lambda t: recv_tile(t).wait_recv())

    for q in range(3):
        f = recv[:, 16 * q : 16 * q + 16, :].reshape(512, LANES)
        o = dot(kr_hi, f) + dot(kr_lo, f)
        back[:, 16 * q : 16 * q + 16, :] = o.astype(BF16).reshape(NE, 16, LANES)

    def send_back(s):
        t = partner(s)
        return pltpu.make_async_remote_copy(
            src_ref=back.at[t], dst_ref=res.at[k], send_sem=bsend.at[t], recv_sem=brecv.at[k],
            device_id=(t, i2, j), device_id_type=MESH,
        )

    def recv_back(t):
        return pltpu.make_async_remote_copy(
            src_ref=back.at[t], dst_ref=res.at[t], send_sem=bsend.at[t], recv_sem=brecv.at[t],
            device_id=(t, i2, j), device_id_type=MESH,
        )

    over(NE, lambda s: send_back(s).start())

    def finish(t):
        recv_back(t).wait_recv()
        big[pl.ds(pl.multiple_of(t * 48, 16), 48), :] = res[t].astype(F32)

    over(NE, finish)
    for v in range(NV):
        out_ref[0, v] = big[pl.ds(v, ROWS, stride=NV), :].astype(BF16)

    over(NE, lambda t: recv_pick(t).wait_send())
    over(NE, lambda t: recv_tile(t).wait_send())
    over(NE, lambda t: recv_back(t).wait_send())
    for di, dj in others:
        send_gram(di, dj).wait_send()


def per_device(x, cw, cb, ow, oi, oc, ov, og):
    vmem = pl.BlockSpec(memory_space=pltpu.VMEM)
    hcol_s, hrow, hcol, obs_r = pl.pallas_call(
        halo_kernel,
        out_shape=(
            jax.ShapeDtypeStruct((2, 2 * NV, LANES), BF16),
            jax.ShapeDtypeStruct((2, 2 * NV, LANES), BF16),
            jax.ShapeDtypeStruct((6, 2 * NV, LANES), BF16),
            jax.ShapeDtypeStruct((8, NOBS), F32),
        ),
        in_specs=[pl.BlockSpec(memory_space=pl.ANY), vmem, vmem, vmem],
        out_specs=(vmem,) * 4,
        scratch_shapes=[
            pltpu.VMEM(x.shape, BF16),
            pltpu.VMEM((NV * PITCH, LANES), F32),
            pltpu.VMEM((2, 2 * NV, LANES), BF16),
            pltpu.VMEM((8, NOBS), F32),
            pltpu.SemaphoreType.DMA,
            pltpu.SemaphoreType.DMA((9,)),
            pltpu.SemaphoreType.DMA((9,)),
        ],
        compiler_params=pltpu.CompilerParams(
            collective_id=0, has_side_effects=True, vmem_limit_bytes=16 * 1024 * 1024
        ),
        cost_estimate=pl.CostEstimate(flops=10**10, bytes_accessed=10**6, transcendentals=0),
        name="halo",
    )(x, oc, ov, og)
    return pl.pallas_call(
        kernel,
        out_shape=jax.ShapeDtypeStruct(x.shape, x.dtype),
        in_specs=[vmem] * 9,
        out_specs=vmem,
        scratch_shapes=[
            pltpu.VMEM((NV * PITCH, LANES), F32),
            pltpu.VMEM((68 * SLAB + 16, LANES), BF16),
            pltpu.VMEM((66 * SLAB + 16, LANES), BF16),
            pltpu.VMEM((256, 256), BF16),
            pltpu.VMEM((32, 256), BF16),
            pltpu.VMEM((NE, 2 * NV, LANES), BF16),
            pltpu.VMEM((NE, 2 * NV, LANES), BF16),
            pltpu.VMEM((NE, 2 * NV, LANES), BF16),
            pltpu.VMEM((NE, 2 * NV, LANES), BF16),
            pltpu.VMEM((1, 1, NOBS), F32),
            pltpu.VMEM((NE, 1, NOBS), F32),
            pltpu.VMEM((16, LANES), F32),
            pltpu.VMEM((NA * NB, 16, LANES), F32),
            pltpu.VMEM((256, 256), BF16),
            pltpu.VMEM((LANES, NOBS), BF16),
            pltpu.VMEM((NE, 512), BF16),
            pltpu.VMEM((2, NE, NE), BF16),
            pltpu.SemaphoreType.DMA((NE,)),
            pltpu.SemaphoreType.DMA((NE,)),
            pltpu.SemaphoreType.DMA((NE,)),
            pltpu.SemaphoreType.DMA((NE,)),
            pltpu.SemaphoreType.DMA((NA * NB,)),
            pltpu.SemaphoreType.DMA((NA * NB,)),
            pltpu.SemaphoreType.DMA((NE,)),
            pltpu.SemaphoreType.DMA((NE,)),
        ],
        compiler_params=pltpu.CompilerParams(
            collective_id=1, has_side_effects=True, vmem_limit_bytes=32 * 1024 * 1024
        ),
        name="cycle",
    )(x, cw, cb.reshape(1, 256), ow.T, oi, hcol_s, hrow, hcol, obs_r)


def solution(mesh):
    return jax.shard_map(
        per_device,
        mesh=mesh,
        in_specs=(
            P("ens", None, "lat", "lon"),
            P(),
            P(),
            P(),
            P("lat", "lon", None),
            P("lat", "lon"),
            P("lat", "lon", None),
            P("lat", "lon", None),
        ),
        out_specs=P("ens", None, "lat", "lon"),
        check_vma=False,
    )
```

```python
import math

import jax
import jax.numpy as jnp
from jax import lax
from jax.experimental import pallas as pl
from jax.experimental.pallas import tpu as pltpu
from jax.sharding import PartitionSpec as P

NS_ITERS = 20
MESH = pl.DeviceIdType.MESH
F32 = jnp.float32
BF16 = jnp.bfloat16
NV = 24
ROWS = 64
LANES = 128
SLAB = 80
NE = 32
NA = 4
NB = 4
PITCH = 72
NOBS = 256


def dot(a, b, dims=((1,), (0,)), precision=None):
    return lax.dot_general(
        a, b, (dims, ((), ())), precision=precision, preferred_element_type=F32
    )


def marks(hit):
    return jnp.where(hit, 1.0, 0.0).astype(BF16)


def lane_iota(shape):
    return lax.broadcasted_iota(jnp.int32, shape, len(shape) - 1)


def row_iota(shape):
    return lax.broadcasted_iota(jnp.int32, shape, len(shape) - 2)


def roll(x, shift):
    if isinstance(shift, int):
        shift = shift % LANES
        if shift == 0:
            return x
    return pltpu.roll(x, shift, 1)


def slab(x, west, east):
    lane = lane_iota((NV, LANES))
    xw = jnp.where(lane == 0, west, roll(x, 1))
    xe = jnp.where(lane == LANES - 1, east, roll(x, -1))
    return jnp.concatenate([xw, x, xe, jnp.ones((8, LANES), F32)], axis=0).astype(BF16)


def gelu2(pre):
    c1 = math.sqrt(2.0 / math.pi)
    c2 = c1 * 0.044715
    x = pre.astype(BF16)
    th = jnp.tanh(x * (jnp.bfloat16(c1) + jnp.bfloat16(c2) * (x * x)))
    return x + x * th


def changes(wt, ow, patches):
    pre = dot(wt, patches)
    return dot(ow, gelu2(pre))


def fill(big, xv):
    for v in range(NV):
        big[v * PITCH : v * PITCH + ROWS, :] = xv[0, v].astype(F32)


def place():
    k = lax.axis_index("ens")
    i = lax.axis_index("lat")
    j = lax.axis_index("lon")

    def peer(dk, di, dj):
        return ((k + dk) % NE, (i + di) % NA, (j + dj) % NB)

    return k, i, j, peer


def meet(peers):
    barrier = pltpu.get_barrier_semaphore()
    for to in peers:
        pl.semaphore_signal(barrier, inc=1, device_id=to, device_id_type=MESH)
    return lambda: pl.semaphore_wait(barrier, len(peers))


def halo_kernel(
    x_hbm, hcol_s, hrow, hcol,
    xv, big, hrow_s, load_sem, hsend, hrecv,
):
    k, i, j, peer = place()
    load = pltpu.make_async_copy(x_hbm, xv, load_sem)
    load.start()
    met = meet(
        [peer(0, di, dj) for di in (0, 1, -1) for dj in (0, 1, -1) if di or dj]
    )
    load.wait()
    lane24 = lane_iota((NV, LANES))

    fill(big, xv)

    def row_of(r):
        return big[pl.ds(r, NV, stride=PITCH), :]

    zero24 = jnp.zeros((NV, LANES), F32)
    cols = (zero24,) * 4
    for row in range(ROWS):
        x = roll(row_of(row), row)
        cols = tuple(
            jnp.where(lane24 == (row + off) % LANES, x, c)
            for c, off in zip(cols, (0, 1, LANES - 2, LANES - 1))
        )
    c0, c1, c126, c127 = cols
    c1 = roll(c1, -1)
    c126 = roll(c126, 2)
    c127 = roll(c127, 1)
    hcol_s[0] = jnp.concatenate([c0, c1], axis=0).astype(BF16)
    hcol_s[1] = jnp.concatenate([c126, c127], axis=0).astype(BF16)
    hrow_s[0] = jnp.concatenate([row_of(0), row_of(1)], axis=0).astype(BF16)
    hrow_s[1] = jnp.concatenate([row_of(ROWS - 2), row_of(ROWS - 1)], axis=0).astype(BF16)
    met()

    def halo(src, dst, n, di, dj):
        return pltpu.make_async_remote_copy(
            src_ref=src, dst_ref=dst, send_sem=hsend.at[n], recv_sem=hrecv.at[n],
            device_id=peer(0, di, dj), device_id_type=MESH,
        )

    north = [
        halo(hrow_s.at[1], hrow.at[0], 0, 1, 0),
        halo(hcol_s.at[1], hcol.at[2], 4, 1, 1),
        halo(hcol_s.at[0], hcol.at[3], 5, 1, -1),
    ]
    south = [
        halo(hrow_s.at[0], hrow.at[1], 1, -1, 0),
        halo(hcol_s.at[1], hcol.at[4], 6, -1, 1),
        halo(hcol_s.at[0], hcol.at[5], 7, -1, -1),
    ]
    sides = [
        halo(hcol_s.at[1], hcol.at[0], 2, 0, 1),
        halo(hcol_s.at[0], hcol.at[1], 3, 0, -1),
    ]

    @pl.when(i < NA - 1)
    def _():
        for c in north:
            c.start()

    @pl.when(i > 0)
    def _():
        for c in south:
            c.start()

    for c in sides:
        c.start()

    @pl.when(i == 0)
    def _():
        hrow[0] = jnp.zeros((2 * NV, LANES), BF16)
        hcol[2] = jnp.zeros((2 * NV, LANES), BF16)
        hcol[3] = jnp.zeros((2 * NV, LANES), BF16)

    @pl.when(i == NA - 1)
    def _():
        hrow[1] = jnp.zeros((2 * NV, LANES), BF16)
        hcol[4] = jnp.zeros((2 * NV, LANES), BF16)
        hcol[5] = jnp.zeros((2 * NV, LANES), BF16)

    for c in sides:
        c.wait()

    @pl.when(i > 0)
    def _():
        for c in north:
            c.wait_recv()

    @pl.when(i < NA - 1)
    def _():
        for c in north:
            c.wait_send()
        for c in south:
            c.wait_recv()

    @pl.when(i > 0)
    def _():
        for c in south:
            c.wait_send()


def kernel(
    xv, cw, cb, ow, oi, oc, ov, og, hcol_s, hrow, hcol, out_ref,
    big, s1, s2, wt, owt,
    fc, recv, back, res, pick_s, hx, gsend, grecv, ep, oh, sp, ets, hs, kr, fr, ob, obs_s, obs_r,
    asend, arecv, psend, precv, gsend_sem, grecv_sem, bsend, brecv, osem,
):
    k, i, j, peer = place()
    i2 = (i + 2) % NA
    k_hi, k_y, k_c = k // 16, (k // 2) % 8, k % 2

    def partner(s):
        s = (s + 1) % NE
        u = s // 4
        dy = ((u + 1) // 2) * (2 * (u % 2) - 1)
        hi = (k_hi + s) % 2
        y = (k_y + 8 + dy) % 8
        c = (k_c + s // 2) % 2
        return hi * 16 + y * 2 + c

    met = meet(
        [peer(0, di, dj) for di in range(NA) for dj in range(NB) if di or dj]
        + [peer(dk, di, 0) for dk in range(1, NE) for di in (0, 2)]
    )
    lane24 = lane_iota((NV, LANES))
    fill(big, xv)

    def row_of(r):
        return big[pl.ds(r, NV, stride=PITCH), :]

    def over(n, body):
        lax.fori_loop(0, n, lambda s, c: (body(s), c)[1], 0)

    w = cw[...].astype(F32)
    b = cb[...]
    b_hi = b.astype(BF16).astype(F32)
    b_mid = (b - b_hi).astype(BF16).astype(F32)
    b_lo = b - b_hi - b_mid
    zeros8 = jnp.zeros((8, 256), F32)
    pad = row_iota((8, 256))
    bias8 = jnp.where(pad == 0, b_hi, jnp.where(pad == 1, b_mid, jnp.where(pad == 2, b_lo, zeros8)))
    wfull = jnp.concatenate(
        [w[0:72], bias8, w[72:144], zeros8, w[144:216], zeros8, zeros8, zeros8], axis=0
    )
    wt[...] = wfull.T.astype(BF16)
    owp = ow[...].astype(F32) * 0.5
    owt[...] = jnp.concatenate([owp, jnp.zeros((8, 256), F32)], axis=0).astype(BF16)
    tail = jnp.zeros((16, LANES), BF16)
    s1[68 * SLAB : 68 * SLAB + 16, :] = tail
    s2[66 * SLAB : 66 * SLAB + 16, :] = tail

    def pair(ref, n):
        both = ref[n].astype(F32)
        return both[0:NV], both[NV : 2 * NV]

    n0, n1 = pair(hrow, 0)
    m0, m1 = pair(hrow, 1)

    def ext(mid, top, bottom):
        out = roll(mid, 2)
        out = jnp.where(lane24 < 2, roll(top, 2 - ROWS), out)
        return jnp.where(lane24 > ROWS + 1, roll(bottom, ROWS + 2), out)

    w_m, w_n, w_s = pair(hcol, 0), pair(hcol, 2), pair(hcol, 4)
    e_m, e_n, e_s = pair(hcol, 1), pair(hcol, 3), pair(hcol, 5)
    cm2 = ext(w_m[0], w_n[0], w_s[0])
    cm1 = ext(w_m[1], w_n[1], w_s[1])
    cp0 = ext(e_m[0], e_n[0], e_s[0])
    cp1 = ext(e_m[1], e_n[1], e_s[1])

    def own(mid, lane):
        out = roll(mid, 2)
        for at, x in ((0, n0), (1, n1), (ROWS + 2, m0), (ROWS + 3, m1)):
            out = jnp.where(lane24 == at, roll(x, at - lane), out)
        return out

    c0e = own(pair(hcol_s, 0)[0], 0)
    c127e = own(pair(hcol_s, 1)[1], LANES - 1)

    def put1(n, x):
        s1[n * SLAB : (n + 1) * SLAB, :] = slab(x, roll(cm1, -n), roll(cp0, LANES - 1 - n))

    for n, x in ((0, n0), (1, n1), (ROWS + 2, m0), (ROWS + 3, m1)):
        put1(n, x)

    for row in range(ROWS):
        put1(row + 2, row_of(row))

    weights = wt[...]
    oweights = owt[...]

    def edge(a0, a1, a2):
        ones = jnp.ones((8, LANES), F32)
        rows = []
        for a in range(3):
            rows += [roll(a0, -a), roll(a1, -a), roll(a2, -a), ones]
        rows.append(jnp.zeros((16, LANES), F32))
        return jnp.concatenate(rows, axis=0).astype(BF16)

    first, last = i > 0, i < NA - 1
    ep[:, 0:LANES] = edge(cm2, cm1, c0e)
    ep[:, LANES : 2 * LANES] = edge(c127e, cp0, cp1)
    ch = changes(weights, oweights, ep[...])
    inside = ((lane24 > 0) | first) & ((lane24 < ROWS + 1) | last)
    mw = jnp.where(inside, roll(cm1, -1) + ch[0:NV, 0:LANES], 0.0)
    me = jnp.where(inside, roll(cp0, -1) + ch[0:NV, LANES : 2 * LANES], 0.0)

    def hide(s, n, q):
        base = pl.multiple_of(n * SLAB, 16)
        p = jnp.concatenate([s[pl.ds(base, 256), :], s[pl.ds(base + SLAB, 256), :]], axis=1)
        hs[q] = gelu2(dot(wt[...], p))

    def tile(s, n, q):
        base = pl.multiple_of(n * SLAB, 16)
        c = dot(owt[...], hs[q])
        mid0 = s[pl.ds(base + SLAB, SLAB), :].astype(F32)[NV : 2 * NV]
        mid1 = s[pl.ds(base + 2 * SLAB, SLAB), :].astype(F32)[NV : 2 * NV]
        return mid0 + c[0:NV, 0:LANES], mid1 + c[0:NV, LANES : 2 * LANES]

    def step1(outer, carry):
        for q in range(11):
            hide(s1, (outer * 11 + q) * 2, q)
        for q in range(11):
            n = (outer * 11 + q) * 2
            for d, m in enumerate(tile(s1, n, q)):
                at = n + d
                keep = ((at > 0) | first) & ((at < ROWS + 1) | last)
                m = jnp.where(keep, m, 0.0)
                s2[pl.ds(pl.multiple_of(at * SLAB, 16), SLAB), :] = slab(
                    m,
                    roll(mw, (LANES - at) % LANES),
                    roll(me, (2 * LANES - 1 - at) % LANES),
                )
        return carry

    lax.fori_loop(0, 3, step1, 0)

    live = (lane_iota((1, NOBS)) < oc[...]).astype(F32)
    obs_s[0:1, :] = ov[0]
    obs_s[1:2, :] = og[0] * live
    obs_s[2:8, :] = jnp.zeros((6, NOBS), F32)

    flat = oi[0]
    v_of, r_of, c_of = flat // 8192, (flat // LANES) % ROWS, flat % LANES
    oh[...] = marks(row_iota((LANES, NOBS)) == c_of)

    def columns(outer):
        rows = pl.ds(pl.multiple_of(outer * (22 * SLAB), 16), 22 * SLAB)
        ob[rows, :] = dot(s2[rows, :], oh[...]).astype(BF16)

    over(3, columns)

    def gather(outer, taps):
        for q in range(11):
            n = outer * 11 + q
            part = ob[pl.ds(pl.multiple_of(n * SLAB, 16), SLAB), :]
            taps = tuple(t + part * marks(r_of == n - a) for a, t in enumerate(taps))
        return taps

    taps = lax.fori_loop(0, 6, gather, (jnp.zeros((SLAB, NOBS), BF16),) * 3)
    for a in range(3):
        ep[a * SLAB : (a + 1) * SLAB, :] = taps[a]
    ep[3 * SLAB : 256, :] = jnp.zeros((16, NOBS), BF16)
    seen = taps[1].astype(F32)[NV : 2 * NV] + changes(weights, oweights, ep[...])[0:NV]
    seen = seen.astype(BF16).astype(F32)
    pick_s[0] = jnp.sum(jnp.where(row_iota((NV, NOBS)) == v_of, seen, 0.0), axis=0, keepdims=True)

    def send_pick(t):
        return pltpu.make_async_remote_copy(
            src_ref=pick_s.at[0], dst_ref=hx.at[k], send_sem=psend.at[t], recv_sem=precv.at[k],
            device_id=(t, i2, j), device_id_type=MESH,
        )

    def send_tile(s):
        t = partner(s)
        return pltpu.make_async_remote_copy(
            src_ref=fc.at[t], dst_ref=recv.at[k], send_sem=asend.at[t], recv_sem=arecv.at[k],
            device_id=(t, i, j), device_id_type=MESH,
        )

    def step2(outer, carry):
        for q in range(8):
            hide(s2, partner(outer * 8 + q) * 2, q)
        for q in range(8):
            s = outer * 8 + q
            t = partner(s)
            f0, f1 = tile(s2, t * 2, q)
            fc[t] = jnp.concatenate([f0, f1], axis=0).astype(BF16)
            if q:
                send_tile(s - 1).start()

        @pl.when(outer < 3)
        def _():
            send_tile(outer * 8 + 7).start()

        return carry

    obs_copy = pltpu.make_async_remote_copy(
        src_ref=obs_s, dst_ref=obs_r, send_sem=osem.at[0], recv_sem=osem.at[1],
        device_id=(k, i2, j), device_id_type=MESH,
    )
    met()
    over(NE, lambda s: send_pick(partner(s)).start())
    obs_copy.start()
    lax.fori_loop(0, 2, step2, 0)

    def recv_pick(t):
        return pltpu.make_async_remote_copy(
            src_ref=pick_s.at[0], dst_ref=hx.at[t], send_sem=psend.at[t], recv_sem=precv.at[t],
            device_id=(t, i2, j), device_id_type=MESH,
        )

    over(NE, lambda t: recv_pick(t).wait_recv())

    values = hx[:, 0, :]
    obs_copy.wait()
    value = obs_r[0:1, :]
    weight = obs_r[1:2, :]
    mean = jnp.mean(values, axis=0, keepdims=True)
    dev = values - mean
    innov = value - mean
    rows40 = jnp.concatenate([dev, jnp.broadcast_to(innov, (8, NOBS))], axis=0)
    wdev = dev * weight
    hp = lax.Precision.HIGHEST
    g4 = dot(rows40, jnp.concatenate([wdev] * 4, axis=0), ((1,), (1,)), hp)
    lane8 = lane_iota((8, LANES))
    packed = jnp.zeros((8, LANES), F32)
    for q in range(4):
        packed = jnp.where(lane8 // 32 == q, g4[8 * q : 8 * q + 8], packed)
    mine = jnp.concatenate([packed, g4[32:40]], axis=0)
    gsend[...] = mine
    slot = i * NB + j
    grecv[slot] = mine

    def send_gram(di, dj):
        n = (di % NA) * NB + dj % NB
        return pltpu.make_async_remote_copy(
            src_ref=gsend, dst_ref=grecv.at[slot], send_sem=gsend_sem.at[n],
            recv_sem=grecv_sem.at[slot], device_id=peer(0, di, dj), device_id_type=MESH,
        )

    def recv_gram(di, dj):
        n = ((i + di) % NA) * NB + (j + dj) % NB
        return pltpu.make_async_remote_copy(
            src_ref=gsend, dst_ref=grecv.at[n], send_sem=gsend_sem.at[0],
            recv_sem=grecv_sem.at[n], device_id=peer(0, di, dj), device_id_type=MESH,
        )

    others = [(di, dj) for di in range(NA) for dj in range(NB) if di or dj]
    for di, dj in others:
        send_gram(di, dj).start()
    lax.fori_loop(2, 4, step2, 0)
    for di, dj in others:
        recv_gram(di, dj).wait_recv()

    total = grecv[0]
    for n in range(1, NA * NB):
        total = total + grecv[n]
    p1, p2 = total[0:8], total[8:16]
    gram = jnp.concatenate(
        [(p1 if q == 0 else roll(p1, -32 * q))[:, 0:32] for q in range(4)], axis=0
    )
    proj = p2[:, 0:32]
    eye = jnp.where(row_iota((NE, NE)) == lane_iota((NE, NE)), 1.0, 0.0)
    system = (NE - 1) * eye + gram

    def full_sum(a):
        return jnp.sum(jnp.sum(a, axis=1, keepdims=True), axis=0, keepdims=True)

    scale = jnp.sqrt(full_sum(system * system))

    current, inverse = system / scale, eye
    for _ in range(NS_ITERS):
        factor = 1.5 * eye - 0.5 * dot(inverse, current, precision=hp)
        new = dot(jnp.concatenate([current, inverse], axis=0), factor, precision=hp)
        current, inverse = new[0:NE], new[NE : 2 * NE]
    root = inverse / jnp.sqrt(scale)
    half = dot(proj, root, precision=hp)
    mean_w = dot(half, root, precision=hp)[0:1]
    full = mean_w + math.sqrt(NE - 1.0) * root
    et = 1.0 / NE + full - jnp.mean(full, axis=1, keepdims=True)
    et_hi = et.astype(BF16)
    et_lo = (et - et_hi.astype(F32)).astype(BF16)

    spread = marks(row_iota((512, NE)) // 16 == lane_iota((512, NE)))
    sp[...] = marks(row_iota((NE, 512)) == lane_iota((NE, 512)) // 16)
    ets[0] = et_hi
    ets[1] = et_lo
    same = row_iota((512, 512)) % 16 == lane_iota((512, 512)) % 16

    def kron(e):
        a = dot(spread, e).astype(BF16)
        return jnp.where(same, dot(a, sp[...]), 0.0).astype(BF16)

    kr[0] = kron(ets[0])
    kr[1] = kron(ets[1])

    def recv_tile(t):
        return pltpu.make_async_remote_copy(
            src_ref=fc.at[t], dst_ref=recv.at[t], send_sem=asend.at[t], recv_sem=arecv.at[t],
            device_id=(t, i, j), device_id_type=MESH,
        )

    recv[k] = fc[k]
    over(NE - 1, lambda s: recv_tile(partner(s)).wait_recv())

    for q in range(3):
        fr[:, q * LANES : (q + 1) * LANES] = recv[:, 16 * q : 16 * q + 16, :].reshape(512, LANES)

    def send_back(t):
        return pltpu.make_async_remote_copy(
            src_ref=back.at[t], dst_ref=res.at[k], send_sem=bsend.at[t], recv_sem=brecv.at[k],
            device_id=(t, i, j), device_id_type=MESH,
        )

    def recv_back(t):
        return pltpu.make_async_remote_copy(
            src_ref=back.at[t], dst_ref=res.at[t], send_sem=bsend.at[t], recv_sem=brecv.at[t],
            device_id=(t, i, j), device_id_type=MESH,
        )

    def group(g):
        return (k // 8 + 1 + g) % 4

    def send_group(g):
        for e in range(8 if g < 3 else 7):
            send_back(group(g) * 8 + (k + 1 + e) % 8).start()

    for g in range(4):
        rows = pl.ds(pl.multiple_of(group(g) * LANES, LANES), LANES)
        o = (dot(kr[0, rows, :], fr[...]) + dot(kr[1, rows, :], fr[...])).astype(BF16)
        for q in range(3):
            back[pl.ds(group(g) * 8, 8), 16 * q : 16 * q + 16, :] = o[
                :, q * LANES : (q + 1) * LANES
            ].reshape(8, 16, LANES)
        if g:
            send_group(g - 1)
    send_group(3)
    res[k] = back[k]

    def finish(s):
        t = partner(s)

        @pl.when(s < NE - 1)
        def _():
            recv_back(t).wait_recv()

        big[pl.ds(pl.multiple_of(t * 48, 16), 48), :] = res[t].astype(F32)

    over(NE, finish)
    for v in range(NV):
        out_ref[0, v] = big[pl.ds(v, ROWS, stride=NV), :].astype(BF16)

    over(NE, lambda t: recv_pick(t).wait_send())
    over(NE - 1, lambda s: recv_tile(partner(s)).wait_send())
    over(NE - 1, lambda s: recv_back(partner(s)).wait_send())
    for di, dj in others:
        send_gram(di, dj).wait_send()


def per_device(x, cw, cb, ow, oi, oc, ov, og):
    vmem = pl.BlockSpec(memory_space=pltpu.VMEM)
    hcol_s, hrow, hcol = pl.pallas_call(
        halo_kernel,
        out_shape=(
            jax.ShapeDtypeStruct((2, 2 * NV, LANES), BF16),
            jax.ShapeDtypeStruct((2, 2 * NV, LANES), BF16),
            jax.ShapeDtypeStruct((6, 2 * NV, LANES), BF16),
        ),
        in_specs=[pl.BlockSpec(memory_space=pl.ANY)],
        out_specs=(vmem,) * 3,
        scratch_shapes=[
            pltpu.VMEM(x.shape, BF16),
            pltpu.VMEM((NV * PITCH, LANES), F32),
            pltpu.VMEM((2, 2 * NV, LANES), BF16),
            pltpu.SemaphoreType.DMA,
            pltpu.SemaphoreType.DMA((9,)),
            pltpu.SemaphoreType.DMA((9,)),
        ],
        compiler_params=pltpu.CompilerParams(
            collective_id=0, has_side_effects=True, vmem_limit_bytes=16 * 1024 * 1024
        ),
        cost_estimate=pl.CostEstimate(flops=10**10, bytes_accessed=10**6, transcendentals=0),
        name="halo",
    )(x)
    return pl.pallas_call(
        kernel,
        out_shape=jax.ShapeDtypeStruct(x.shape, x.dtype),
        in_specs=[vmem] * 11,
        out_specs=vmem,
        scratch_shapes=[
            pltpu.VMEM((NV * PITCH, LANES), F32),
            pltpu.VMEM((68 * SLAB + 16, LANES), BF16),
            pltpu.VMEM((66 * SLAB + 16, LANES), BF16),
            pltpu.VMEM((256, 256), BF16),
            pltpu.VMEM((32, 256), BF16),
            pltpu.VMEM((NE, 2 * NV, LANES), BF16),
            pltpu.VMEM((NE, 2 * NV, LANES), BF16),
            pltpu.VMEM((NE, 2 * NV, LANES), BF16),
            pltpu.VMEM((NE, 2 * NV, LANES), BF16),
            pltpu.VMEM((1, 1, NOBS), F32),
            pltpu.VMEM((NE, 1, NOBS), F32),
            pltpu.VMEM((16, LANES), F32),
            pltpu.VMEM((NA * NB, 16, LANES), F32),
            pltpu.VMEM((256, 256), BF16),
            pltpu.VMEM((LANES, NOBS), BF16),
            pltpu.VMEM((NE, 512), BF16),
            pltpu.VMEM((2, NE, NE), BF16),
            pltpu.VMEM((11, 256, 256), BF16),
            pltpu.VMEM((2, 512, 512), BF16),
            pltpu.VMEM((512, 3 * LANES), BF16),
            pltpu.VMEM((66 * SLAB, NOBS), BF16),
            pltpu.VMEM((8, NOBS), F32),
            pltpu.VMEM((8, NOBS), F32),
            pltpu.SemaphoreType.DMA((NE,)),
            pltpu.SemaphoreType.DMA((NE,)),
            pltpu.SemaphoreType.DMA((NE,)),
            pltpu.SemaphoreType.DMA((NE,)),
            pltpu.SemaphoreType.DMA((NA * NB,)),
            pltpu.SemaphoreType.DMA((NA * NB,)),
            pltpu.SemaphoreType.DMA((NE,)),
            pltpu.SemaphoreType.DMA((NE,)),
            pltpu.SemaphoreType.DMA((2,)),
        ],
        compiler_params=pltpu.CompilerParams(
            collective_id=1, has_side_effects=True, vmem_limit_bytes=32 * 1024 * 1024
        ),
        name="cycle",
    )(x, cw, cb.reshape(1, 256), ow.T, oi, oc, ov, og, hcol_s, hrow, hcol)


def solution(mesh):
    return jax.shard_map(
        per_device,
        mesh=mesh,
        in_specs=(
            P("ens", None, "lat", "lon"),
            P(),
            P(),
            P(),
            P("lat", "lon", None),
            P("lat", "lon"),
            P("lat", "lon", None),
            P("lat", "lon", None),
        ),
        out_specs=P("ens", None, "lat", "lon"),
        check_vma=False,
    )
```

```python
import math

import jax
import jax.numpy as jnp
from jax import lax
from jax.experimental import pallas as pl
from jax.experimental.pallas import tpu as pltpu
from jax.sharding import PartitionSpec as P

NS_ITERS = 20
MESH = pl.DeviceIdType.MESH
F32 = jnp.float32
BF16 = jnp.bfloat16
NV = 24
ROWS = 64
LANES = 128
SLAB = 80
NE = 32
NA = 4
NB = 4
PITCH = 72
NOBS = 256


def dot(a, b, dims=((1,), (0,)), precision=None):
    return lax.dot_general(
        a, b, (dims, ((), ())), precision=precision, preferred_element_type=F32
    )


def marks(hit):
    return jnp.where(hit, 1.0, 0.0).astype(BF16)


def lane_iota(shape):
    return lax.broadcasted_iota(jnp.int32, shape, len(shape) - 1)


def row_iota(shape):
    return lax.broadcasted_iota(jnp.int32, shape, len(shape) - 2)


def roll(x, shift):
    if isinstance(shift, int):
        shift = shift % LANES
        if shift == 0:
            return x
    return pltpu.roll(x, shift, 1)


def slab(x, west, east):
    lane = lane_iota((NV, LANES))
    xw = jnp.where(lane == 0, west, roll(x, 1))
    xe = jnp.where(lane == LANES - 1, east, roll(x, -1))
    return jnp.concatenate([xw, x, xe, jnp.ones((8, LANES), F32)], axis=0).astype(BF16)


def gelu2(pre):
    c1 = math.sqrt(2.0 / math.pi)
    c2 = c1 * 0.044715
    x = pre.astype(BF16)
    th = jnp.tanh(x * (jnp.bfloat16(c1) + jnp.bfloat16(c2) * (x * x)))
    return x + x * th


def changes(wt, ow, patches):
    pre = dot(wt, patches)
    return dot(ow, gelu2(pre))


def fill(big, xv):
    for v in range(NV):
        big[v * PITCH : v * PITCH + ROWS, :] = xv[0, v].astype(F32)


def place():
    k = lax.axis_index("ens")
    i = lax.axis_index("lat")
    j = lax.axis_index("lon")

    def peer(dk, di, dj):
        return ((k + dk) % NE, (i + di) % NA, (j + dj) % NB)

    return k, i, j, peer


def meet(peers):
    barrier = pltpu.get_barrier_semaphore()
    for to in peers:
        pl.semaphore_signal(barrier, inc=1, device_id=to, device_id_type=MESH)
    return lambda: pl.semaphore_wait(barrier, len(peers))


def halo_kernel(
    x_hbm, hcol_s, hrow, hcol,
    xv, big, hrow_s, load_sem, hsend, hrecv,
):
    k, i, j, peer = place()
    load = pltpu.make_async_copy(x_hbm, xv, load_sem)
    load.start()
    met = meet(
        [peer(0, di, dj) for di in (0, 1, -1) for dj in (0, 1, -1) if di or dj]
    )
    load.wait()
    lane24 = lane_iota((NV, LANES))

    fill(big, xv)

    def row_of(r):
        return big[pl.ds(r, NV, stride=PITCH), :]

    zero24 = jnp.zeros((NV, LANES), F32)
    cols = (zero24,) * 4
    for row in range(ROWS):
        x = roll(row_of(row), row)
        cols = tuple(
            jnp.where(lane24 == (row + off) % LANES, x, c)
            for c, off in zip(cols, (0, 1, LANES - 2, LANES - 1))
        )
    c0, c1, c126, c127 = cols
    c1 = roll(c1, -1)
    c126 = roll(c126, 2)
    c127 = roll(c127, 1)
    hcol_s[0] = jnp.concatenate([c0, c1], axis=0).astype(BF16)
    hcol_s[1] = jnp.concatenate([c126, c127], axis=0).astype(BF16)
    hrow_s[0] = jnp.concatenate([row_of(0), row_of(1)], axis=0).astype(BF16)
    hrow_s[1] = jnp.concatenate([row_of(ROWS - 2), row_of(ROWS - 1)], axis=0).astype(BF16)
    met()

    def halo(src, dst, n, di, dj):
        return pltpu.make_async_remote_copy(
            src_ref=src, dst_ref=dst, send_sem=hsend.at[n], recv_sem=hrecv.at[n],
            device_id=peer(0, di, dj), device_id_type=MESH,
        )

    north = [
        halo(hrow_s.at[1], hrow.at[0], 0, 1, 0),
        halo(hcol_s.at[1], hcol.at[2], 4, 1, 1),
        halo(hcol_s.at[0], hcol.at[3], 5, 1, -1),
    ]
    south = [
        halo(hrow_s.at[0], hrow.at[1], 1, -1, 0),
        halo(hcol_s.at[1], hcol.at[4], 6, -1, 1),
        halo(hcol_s.at[0], hcol.at[5], 7, -1, -1),
    ]
    sides = [
        halo(hcol_s.at[1], hcol.at[0], 2, 0, 1),
        halo(hcol_s.at[0], hcol.at[1], 3, 0, -1),
    ]

    @pl.when(i < NA - 1)
    def _():
        for c in north:
            c.start()

    @pl.when(i > 0)
    def _():
        for c in south:
            c.start()

    for c in sides:
        c.start()

    @pl.when(i == 0)
    def _():
        hrow[0] = jnp.zeros((2 * NV, LANES), BF16)
        hcol[2] = jnp.zeros((2 * NV, LANES), BF16)
        hcol[3] = jnp.zeros((2 * NV, LANES), BF16)

    @pl.when(i == NA - 1)
    def _():
        hrow[1] = jnp.zeros((2 * NV, LANES), BF16)
        hcol[4] = jnp.zeros((2 * NV, LANES), BF16)
        hcol[5] = jnp.zeros((2 * NV, LANES), BF16)

    for c in sides:
        c.wait()

    @pl.when(i > 0)
    def _():
        for c in north:
            c.wait_recv()

    @pl.when(i < NA - 1)
    def _():
        for c in north:
            c.wait_send()
        for c in south:
            c.wait_recv()

    @pl.when(i > 0)
    def _():
        for c in south:
            c.wait_send()


def kernel(
    xv, cw, cb, ow, oi, oc, ov, og, hcol_s, hrow, hcol, out_ref,
    big, s1, s2, wt, owt,
    fc, recv, back, res, pick_s, hx, gsend, grecv, ep, oh, sp, ets, hs, kr, fr, ob, obs_s, obs_r,
    asend, arecv, psend, precv, gsend_sem, grecv_sem, bsend, brecv, osem,
):
    k, i, j, peer = place()
    i2 = (i + 2) % NA
    k_hi, k_y, k_c = k // 16, (k // 2) % 8, k % 2

    def partner(s):
        s = (s + 1) % NE
        u = s // 4
        dy = ((u + 1) // 2) * (2 * (u % 2) - 1)
        hi = (k_hi + s) % 2
        y = (k_y + 8 + dy) % 8
        c = (k_c + s // 2) % 2
        return hi * 16 + y * 2 + c

    met = meet(
        [peer(0, di, dj) for di in range(NA) for dj in range(NB) if di or dj]
        + [peer(dk, di, 0) for dk in range(1, NE) for di in (0, 2)]
    )
    lane24 = lane_iota((NV, LANES))
    fill(big, xv)

    def row_of(r):
        return big[pl.ds(r, NV, stride=PITCH), :]

    def over(n, body):
        lax.fori_loop(0, n, lambda s, c: (body(s), c)[1], 0)

    w = cw[...].astype(F32)
    b = cb[...]
    b_hi = b.astype(BF16).astype(F32)
    b_mid = (b - b_hi).astype(BF16).astype(F32)
    b_lo = b - b_hi - b_mid
    zeros8 = jnp.zeros((8, 256), F32)
    pad = row_iota((8, 256))
    bias8 = jnp.where(pad == 0, b_hi, jnp.where(pad == 1, b_mid, jnp.where(pad == 2, b_lo, zeros8)))
    wfull = jnp.concatenate(
        [w[0:72], bias8, w[72:144], zeros8, w[144:216], zeros8, zeros8, zeros8], axis=0
    )
    wt[...] = wfull.T.astype(BF16)
    owp = ow[...].astype(F32) * 0.5
    owt[...] = jnp.concatenate([owp, jnp.zeros((8, 256), F32)], axis=0).astype(BF16)
    tail = jnp.zeros((16, LANES), BF16)
    s1[68 * SLAB : 68 * SLAB + 16, :] = tail
    s2[66 * SLAB : 66 * SLAB + 16, :] = tail

    def pair(ref, n):
        both = ref[n].astype(F32)
        return both[0:NV], both[NV : 2 * NV]

    n0, n1 = pair(hrow, 0)
    m0, m1 = pair(hrow, 1)

    def ext(mid, top, bottom):
        out = roll(mid, 2)
        out = jnp.where(lane24 < 2, roll(top, 2 - ROWS), out)
        return jnp.where(lane24 > ROWS + 1, roll(bottom, ROWS + 2), out)

    w_m, w_n, w_s = pair(hcol, 0), pair(hcol, 2), pair(hcol, 4)
    e_m, e_n, e_s = pair(hcol, 1), pair(hcol, 3), pair(hcol, 5)
    cm2 = ext(w_m[0], w_n[0], w_s[0])
    cm1 = ext(w_m[1], w_n[1], w_s[1])
    cp0 = ext(e_m[0], e_n[0], e_s[0])
    cp1 = ext(e_m[1], e_n[1], e_s[1])

    def own(mid, lane):
        out = roll(mid, 2)
        for at, x in ((0, n0), (1, n1), (ROWS + 2, m0), (ROWS + 3, m1)):
            out = jnp.where(lane24 == at, roll(x, at - lane), out)
        return out

    c0e = own(pair(hcol_s, 0)[0], 0)
    c127e = own(pair(hcol_s, 1)[1], LANES - 1)

    def put1(n, x):
        s1[n * SLAB : (n + 1) * SLAB, :] = slab(x, roll(cm1, -n), roll(cp0, LANES - 1 - n))

    for n, x in ((0, n0), (1, n1), (ROWS + 2, m0), (ROWS + 3, m1)):
        put1(n, x)

    for row in range(ROWS):
        put1(row + 2, row_of(row))

    weights = wt[...]
    oweights = owt[...]

    def edge(a0, a1, a2):
        ones = jnp.ones((8, LANES), F32)
        rows = []
        for a in range(3):
            rows += [roll(a0, -a), roll(a1, -a), roll(a2, -a), ones]
        rows.append(jnp.zeros((16, LANES), F32))
        return jnp.concatenate(rows, axis=0).astype(BF16)

    first, last = i > 0, i < NA - 1
    ep[:, 0:LANES] = edge(cm2, cm1, c0e)
    ep[:, LANES : 2 * LANES] = edge(c127e, cp0, cp1)
    ch = changes(weights, oweights, ep[...])
    inside = ((lane24 > 0) | first) & ((lane24 < ROWS + 1) | last)
    mw = jnp.where(inside, roll(cm1, -1) + ch[0:NV, 0:LANES], 0.0)
    me = jnp.where(inside, roll(cp0, -1) + ch[0:NV, LANES : 2 * LANES], 0.0)

    def hide(s, n, q):
        base = pl.multiple_of(n * SLAB, 16)
        p = jnp.concatenate([s[pl.ds(base, 256), :], s[pl.ds(base + SLAB, 256), :]], axis=1)
        hs[q] = gelu2(dot(wt[...], p))

    def tile(s, n, q):
        base = pl.multiple_of(n * SLAB, 16)
        c = dot(owt[...], hs[q])
        mid0 = s[pl.ds(base + SLAB, SLAB), :].astype(F32)[NV : 2 * NV]
        mid1 = s[pl.ds(base + 2 * SLAB, SLAB), :].astype(F32)[NV : 2 * NV]
        return mid0 + c[0:NV, 0:LANES], mid1 + c[0:NV, LANES : 2 * LANES]

    def step1(outer, carry):
        for q in range(11):
            hide(s1, (outer * 11 + q) * 2, q)
        for q in range(11):
            n = (outer * 11 + q) * 2
            for d, m in enumerate(tile(s1, n, q)):
                at = n + d
                keep = ((at > 0) | first) & ((at < ROWS + 1) | last)
                m = jnp.where(keep, m, 0.0)
                s2[pl.ds(pl.multiple_of(at * SLAB, 16), SLAB), :] = slab(
                    m,
                    roll(mw, (LANES - at) % LANES),
                    roll(me, (2 * LANES - 1 - at) % LANES),
                )
        return carry

    lax.fori_loop(0, 3, step1, 0)

    live = (lane_iota((1, NOBS)) < oc[...]).astype(F32)
    obs_s[0:1, :] = ov[0]
    obs_s[1:2, :] = og[0] * live
    obs_s[2:8, :] = jnp.zeros((6, NOBS), F32)

    flat = oi[0]
    v_of, r_of, c_of = flat // 8192, (flat // LANES) % ROWS, flat % LANES
    oh[...] = marks(row_iota((LANES, NOBS)) == c_of)

    def columns(outer):
        rows = pl.ds(pl.multiple_of(outer * (22 * SLAB), 16), 22 * SLAB)
        ob[rows, :] = dot(s2[rows, :], oh[...]).astype(BF16)

    over(3, columns)

    def gather(outer, taps):
        for q in range(11):
            n = outer * 11 + q
            part = ob[pl.ds(pl.multiple_of(n * SLAB, 16), SLAB), :]
            taps = tuple(t + part * marks(r_of == n - a) for a, t in enumerate(taps))
        return taps

    taps = lax.fori_loop(0, 6, gather, (jnp.zeros((SLAB, NOBS), BF16),) * 3)
    for a in range(3):
        ep[a * SLAB : (a + 1) * SLAB, :] = taps[a]
    ep[3 * SLAB : 256, :] = jnp.zeros((16, NOBS), BF16)
    seen = taps[1].astype(F32)[NV : 2 * NV] + changes(weights, oweights, ep[...])[0:NV]
    seen = seen.astype(BF16).astype(F32)
    pick_s[0] = jnp.sum(jnp.where(row_iota((NV, NOBS)) == v_of, seen, 0.0), axis=0, keepdims=True)

    def send_pick(t):
        return pltpu.make_async_remote_copy(
            src_ref=pick_s.at[0], dst_ref=hx.at[k], send_sem=psend.at[t], recv_sem=precv.at[k],
            device_id=(t, i2, j), device_id_type=MESH,
        )

    def send_tile(s):
        t = partner(s)
        return pltpu.make_async_remote_copy(
            src_ref=fc.at[t], dst_ref=recv.at[k], send_sem=asend.at[t], recv_sem=arecv.at[k],
            device_id=(t, i, j), device_id_type=MESH,
        )

    def step2(outer, carry):
        for q in range(8):
            hide(s2, partner(outer * 8 + q) * 2, q)
        for q in range(8):
            s = outer * 8 + q
            t = partner(s)
            f0, f1 = tile(s2, t * 2, q)
            fc[t] = jnp.concatenate([f0, f1], axis=0).astype(BF16)
        return carry

    obs_copy = pltpu.make_async_remote_copy(
        src_ref=obs_s, dst_ref=obs_r, send_sem=osem.at[0], recv_sem=osem.at[1],
        device_id=(k, i2, j), device_id_type=MESH,
    )
    met()
    over(NE, lambda s: send_pick(partner(s)).start())
    obs_copy.start()
    lax.fori_loop(0, 1, step2, 0)
    over(8, lambda s: send_tile(s).start())
    lax.fori_loop(1, 4, step2, 0)

    def recv_pick(t):
        return pltpu.make_async_remote_copy(
            src_ref=pick_s.at[0], dst_ref=hx.at[t], send_sem=psend.at[t], recv_sem=precv.at[t],
            device_id=(t, i2, j), device_id_type=MESH,
        )

    over(NE, lambda t: recv_pick(t).wait_recv())

    values = hx[:, 0, :]
    obs_copy.wait()
    value = obs_r[0:1, :]
    weight = obs_r[1:2, :]
    mean = jnp.mean(values, axis=0, keepdims=True)
    dev = values - mean
    innov = value - mean
    rows40 = jnp.concatenate([dev, jnp.broadcast_to(innov, (8, NOBS))], axis=0)
    wdev = dev * weight
    hp = lax.Precision.HIGHEST
    g4 = dot(rows40, jnp.concatenate([wdev] * 4, axis=0), ((1,), (1,)), hp)
    lane8 = lane_iota((8, LANES))
    packed = jnp.zeros((8, LANES), F32)
    for q in range(4):
        packed = jnp.where(lane8 // 32 == q, g4[8 * q : 8 * q + 8], packed)
    row8 = row_iota((8, LANES))
    spare = (
        ((row8 == 0) & (lane8 > 1) & (lane8 < NE))
        | ((row8 == 1) & (lane8 == 0))
        | ((row8 == 2) & (lane8 == 1))
    )
    mine = jnp.where(spare, g4[32:40], packed)
    gsend[...] = mine
    slot = i * NB + j
    grecv[slot] = mine

    def send_gram(di, dj):
        n = (di % NA) * NB + dj % NB
        return pltpu.make_async_remote_copy(
            src_ref=gsend, dst_ref=grecv.at[slot], send_sem=gsend_sem.at[n],
            recv_sem=grecv_sem.at[slot], device_id=peer(0, di, dj), device_id_type=MESH,
        )

    def recv_gram(di, dj):
        n = ((i + di) % NA) * NB + (j + dj) % NB
        return pltpu.make_async_remote_copy(
            src_ref=gsend, dst_ref=grecv.at[n], send_sem=gsend_sem.at[0],
            recv_sem=grecv_sem.at[n], device_id=peer(0, di, dj), device_id_type=MESH,
        )

    others = [(di, dj) for di in range(NA) for dj in range(NB) if di or dj]
    for di, dj in others:
        send_gram(di, dj).start()
    over(NE - 9, lambda s: send_tile(s + 8).start())
    for di, dj in others:
        recv_gram(di, dj).wait_recv()

    total = grecv[0]
    for n in range(1, NA * NB):
        total = total + grecv[n]
    square = jnp.concatenate([roll(total, -32 * q)[:, 0:NE] for q in range(4)], axis=0)
    row32, lane32 = row_iota((NE, NE)), lane_iota((NE, NE))
    taken = (
        ((row32 == 0) & (lane32 > 1))
        | ((row32 == 1) & (lane32 == 0))
        | ((row32 == 2) & (lane32 == 1))
    )
    gram = jnp.where(taken, square.T, square)
    lane1 = lane_iota((1, NE))
    proj = jnp.where(lane1 == 0, square[1:2], jnp.where(lane1 == 1, square[2:3], square[0:1]))
    proj = jnp.broadcast_to(proj, (8, NE))
    eye = jnp.where(row_iota((NE, NE)) == lane_iota((NE, NE)), 1.0, 0.0)
    system = (NE - 1) * eye + gram

    def full_sum(a):
        return jnp.sum(jnp.sum(a, axis=1, keepdims=True), axis=0, keepdims=True)

    scale = jnp.sqrt(full_sum(system * system))

    current = system / scale
    inverse = 1.5 * eye - 0.5 * current
    current = dot(current, inverse, precision=hp)
    for _ in range(NS_ITERS - 1):
        factor = 1.5 * eye - 0.5 * dot(inverse, current, precision=hp)
        current, inverse = dot(current, factor, precision=hp), dot(factor, inverse, precision=hp)
    root = inverse / jnp.sqrt(scale)
    half = dot(proj, root, precision=hp)
    mean_w = dot(half, root, precision=hp)[0:1]
    full = mean_w + math.sqrt(NE - 1.0) * root
    et = 1.0 / NE + full - jnp.mean(full, axis=1, keepdims=True)
    et_hi = et.astype(BF16)
    et_lo = (et - et_hi.astype(F32)).astype(BF16)

    spread = marks(row_iota((512, NE)) // 16 == lane_iota((512, NE)))
    sp[...] = marks(row_iota((NE, 512)) == lane_iota((NE, 512)) // 16)
    ets[0] = et_hi
    ets[1] = et_lo
    same = row_iota((512, 512)) % 16 == lane_iota((512, 512)) % 16

    def kron(e):
        a = dot(spread, e).astype(BF16)
        return jnp.where(same, dot(a, sp[...]), 0.0).astype(BF16)

    kr[0] = kron(ets[0])
    kr[1] = kron(ets[1])

    def recv_tile(t):
        return pltpu.make_async_remote_copy(
            src_ref=fc.at[t], dst_ref=recv.at[t], send_sem=asend.at[t], recv_sem=arecv.at[t],
            device_id=(t, i, j), device_id_type=MESH,
        )

    recv[k] = fc[k]
    over(NE - 1, lambda s: recv_tile(partner(s)).wait_recv())

    for q in range(3):
        fr[:, q * LANES : (q + 1) * LANES] = recv[:, 16 * q : 16 * q + 16, :].reshape(512, LANES)

    def send_back(t):
        return pltpu.make_async_remote_copy(
            src_ref=back.at[t], dst_ref=res.at[k], send_sem=bsend.at[t], recv_sem=brecv.at[k],
            device_id=(t, i, j), device_id_type=MESH,
        )

    def recv_back(t):
        return pltpu.make_async_remote_copy(
            src_ref=back.at[t], dst_ref=res.at[t], send_sem=bsend.at[t], recv_sem=brecv.at[t],
            device_id=(t, i, j), device_id_type=MESH,
        )

    def group(g):
        return (k // 8 + 1 + g) % 4

    def send_group(g):
        for e in range(8 if g < 3 else 7):
            send_back(group(g) * 8 + (k + 1 + e) % 8).start()

    for g in range(4):
        rows = pl.ds(pl.multiple_of(group(g) * LANES, LANES), LANES)
        o = (dot(kr[0, rows, :], fr[...]) + dot(kr[1, rows, :], fr[...])).astype(BF16)
        for q in range(3):
            back[pl.ds(group(g) * 8, 8), 16 * q : 16 * q + 16, :] = o[
                :, q * LANES : (q + 1) * LANES
            ].reshape(8, 16, LANES)
        if g:
            send_group(g - 1)
    send_group(3)
    res[k] = back[k]

    def finish(s):
        t = partner(s)

        @pl.when(s < NE - 1)
        def _():
            recv_back(t).wait_recv()

        big[pl.ds(pl.multiple_of(t * 48, 16), 48), :] = res[t].astype(F32)

    over(NE, finish)
    for v in range(NV):
        out_ref[0, v] = big[pl.ds(v, ROWS, stride=NV), :].astype(BF16)

    over(NE, lambda t: recv_pick(t).wait_send())
    over(NE - 1, lambda s: recv_tile(partner(s)).wait_send())
    over(NE - 1, lambda s: recv_back(partner(s)).wait_send())
    for di, dj in others:
        send_gram(di, dj).wait_send()


def per_device(x, cw, cb, ow, oi, oc, ov, og):
    vmem = pl.BlockSpec(memory_space=pltpu.VMEM)
    hcol_s, hrow, hcol = pl.pallas_call(
        halo_kernel,
        out_shape=(
            jax.ShapeDtypeStruct((2, 2 * NV, LANES), BF16),
            jax.ShapeDtypeStruct((2, 2 * NV, LANES), BF16),
            jax.ShapeDtypeStruct((6, 2 * NV, LANES), BF16),
        ),
        in_specs=[pl.BlockSpec(memory_space=pl.ANY)],
        out_specs=(vmem,) * 3,
        scratch_shapes=[
            pltpu.VMEM(x.shape, BF16),
            pltpu.VMEM((NV * PITCH, LANES), F32),
            pltpu.VMEM((2, 2 * NV, LANES), BF16),
            pltpu.SemaphoreType.DMA,
            pltpu.SemaphoreType.DMA((9,)),
            pltpu.SemaphoreType.DMA((9,)),
        ],
        compiler_params=pltpu.CompilerParams(
            collective_id=0, has_side_effects=True, vmem_limit_bytes=16 * 1024 * 1024
        ),
        cost_estimate=pl.CostEstimate(flops=10**10, bytes_accessed=10**6, transcendentals=0),
        name="halo",
    )(x)
    return pl.pallas_call(
        kernel,
        out_shape=jax.ShapeDtypeStruct(x.shape, x.dtype),
        in_specs=[vmem] * 11,
        out_specs=vmem,
        scratch_shapes=[
            pltpu.VMEM((NV * PITCH, LANES), F32),
            pltpu.VMEM((68 * SLAB + 16, LANES), BF16),
            pltpu.VMEM((66 * SLAB + 16, LANES), BF16),
            pltpu.VMEM((256, 256), BF16),
            pltpu.VMEM((32, 256), BF16),
            pltpu.VMEM((NE, 2 * NV, LANES), BF16),
            pltpu.VMEM((NE, 2 * NV, LANES), BF16),
            pltpu.VMEM((NE, 2 * NV, LANES), BF16),
            pltpu.VMEM((NE, 2 * NV, LANES), BF16),
            pltpu.VMEM((1, 1, NOBS), F32),
            pltpu.VMEM((NE, 1, NOBS), F32),
            pltpu.VMEM((8, LANES), F32),
            pltpu.VMEM((NA * NB, 8, LANES), F32),
            pltpu.VMEM((256, 256), BF16),
            pltpu.VMEM((LANES, NOBS), BF16),
            pltpu.VMEM((NE, 512), BF16),
            pltpu.VMEM((2, NE, NE), BF16),
            pltpu.VMEM((11, 256, 256), BF16),
            pltpu.VMEM((2, 512, 512), BF16),
            pltpu.VMEM((512, 3 * LANES), BF16),
            pltpu.VMEM((66 * SLAB, NOBS), BF16),
            pltpu.VMEM((8, NOBS), F32),
            pltpu.VMEM((8, NOBS), F32),
            pltpu.SemaphoreType.DMA((NE,)),
            pltpu.SemaphoreType.DMA((NE,)),
            pltpu.SemaphoreType.DMA((NE,)),
            pltpu.SemaphoreType.DMA((NE,)),
            pltpu.SemaphoreType.DMA((NA * NB,)),
            pltpu.SemaphoreType.DMA((NA * NB,)),
            pltpu.SemaphoreType.DMA((NE,)),
            pltpu.SemaphoreType.DMA((NE,)),
            pltpu.SemaphoreType.DMA((2,)),
        ],
        compiler_params=pltpu.CompilerParams(
            collective_id=1, has_side_effects=True, vmem_limit_bytes=32 * 1024 * 1024
        ),
        name="cycle",
    )(x, cw, cb.reshape(1, 256), ow.T, oi, oc, ov, og, hcol_s, hrow, hcol)


def solution(mesh):
    return jax.shard_map(
        per_device,
        mesh=mesh,
        in_specs=(
            P("ens", None, "lat", "lon"),
            P(),
            P(),
            P(),
            P("lat", "lon", None),
            P("lat", "lon"),
            P("lat", "lon", None),
            P("lat", "lon", None),
        ),
        out_specs=P("ens", None, "lat", "lon"),
        check_vma=False,
    )
```

```python
import math

import jax
import jax.numpy as jnp
from jax import lax
from jax.experimental import pallas as pl
from jax.experimental.pallas import tpu as pltpu
from jax.sharding import PartitionSpec as P

NS_ITERS = 20
MESH = pl.DeviceIdType.MESH
F32 = jnp.float32
BF16 = jnp.bfloat16
NV = 24
ROWS = 64
LANES = 128
SLAB = 80
NE = 32
NA = 4
NB = 4
PITCH = 72
NOBS = 256


def dot(a, b, dims=((1,), (0,)), precision=None):
    return lax.dot_general(
        a, b, (dims, ((), ())), precision=precision, preferred_element_type=F32
    )


def marks(hit):
    return jnp.where(hit, 1.0, 0.0).astype(BF16)


def lane_iota(shape):
    return lax.broadcasted_iota(jnp.int32, shape, len(shape) - 1)


def row_iota(shape):
    return lax.broadcasted_iota(jnp.int32, shape, len(shape) - 2)


def roll(x, shift):
    if isinstance(shift, int):
        shift = shift % LANES
        if shift == 0:
            return x
    return pltpu.roll(x, shift, 1)


def slab(x, west, east):
    lane = lane_iota((NV, LANES))
    xw = jnp.where(lane == 0, west, roll(x, 1))
    xe = jnp.where(lane == LANES - 1, east, roll(x, -1))
    return jnp.concatenate([xw, x, xe, jnp.ones((8, LANES), F32)], axis=0).astype(BF16)


def gelu2(pre):
    c1 = math.sqrt(2.0 / math.pi)
    c2 = c1 * 0.044715
    x = pre.astype(BF16)
    th = jnp.tanh(x * (jnp.bfloat16(c1) + jnp.bfloat16(c2) * (x * x)))
    return x + x * th


def changes(wt, ow, patches):
    pre = dot(wt, patches)
    return dot(ow, gelu2(pre))


def fill(big, xv):
    for v in range(NV):
        big[v * PITCH : v * PITCH + ROWS, :] = xv[0, v].astype(F32)


def place():
    k = lax.axis_index("ens")
    i = lax.axis_index("lat")
    j = lax.axis_index("lon")

    def peer(dk, di, dj):
        return tuple(
            at if d % n == 0 else lax.rem(at + d % n, n)
            for at, d, n in ((k, dk, NE), (i, di, NA), (j, dj, NB))
        )

    return k, i, j, peer


def meet(peers):
    barrier = pltpu.get_barrier_semaphore()
    for to in peers:
        pl.semaphore_signal(barrier, inc=1, device_id=to, device_id_type=MESH)
    return lambda: pl.semaphore_wait(barrier, len(peers))


def halo_kernel(
    x_hbm, hcol_s, hrow, hcol,
    xv, big, hrow_s, load_sem, hsend, hrecv,
):
    k, i, j, peer = place()
    load = pltpu.make_async_copy(x_hbm, xv, load_sem)
    load.start()
    met = meet(
        [peer(0, di, dj) for di in (0, 1, -1) for dj in (0, 1, -1) if di or dj]
    )
    load.wait()
    lane24 = lane_iota((NV, LANES))

    fill(big, xv)

    def row_of(r):
        return big[pl.ds(r, NV, stride=PITCH), :]

    zero24 = jnp.zeros((NV, LANES), F32)
    cols = (zero24,) * 4
    for row in range(ROWS):
        x = roll(row_of(row), row)
        cols = tuple(
            jnp.where(lane24 == (row + off) % LANES, x, c)
            for c, off in zip(cols, (0, 1, LANES - 2, LANES - 1))
        )
    c0, c1, c126, c127 = cols
    c1 = roll(c1, -1)
    c126 = roll(c126, 2)
    c127 = roll(c127, 1)
    hcol_s[0] = jnp.concatenate([c0, c1], axis=0).astype(BF16)
    hcol_s[1] = jnp.concatenate([c126, c127], axis=0).astype(BF16)
    hrow_s[0] = jnp.concatenate([row_of(0), row_of(1)], axis=0).astype(BF16)
    hrow_s[1] = jnp.concatenate([row_of(ROWS - 2), row_of(ROWS - 1)], axis=0).astype(BF16)
    met()

    def halo(src, dst, n, di, dj):
        return pltpu.make_async_remote_copy(
            src_ref=src, dst_ref=dst, send_sem=hsend.at[n], recv_sem=hrecv.at[n],
            device_id=peer(0, di, dj), device_id_type=MESH,
        )

    north = [
        halo(hrow_s.at[1], hrow.at[0], 0, 1, 0),
        halo(hcol_s.at[1], hcol.at[2], 4, 1, 1),
        halo(hcol_s.at[0], hcol.at[3], 5, 1, -1),
    ]
    south = [
        halo(hrow_s.at[0], hrow.at[1], 1, -1, 0),
        halo(hcol_s.at[1], hcol.at[4], 6, -1, 1),
        halo(hcol_s.at[0], hcol.at[5], 7, -1, -1),
    ]
    sides = [
        halo(hcol_s.at[1], hcol.at[0], 2, 0, 1),
        halo(hcol_s.at[0], hcol.at[1], 3, 0, -1),
    ]

    @pl.when(i < NA - 1)
    def _():
        for c in north:
            c.start()

    @pl.when(i > 0)
    def _():
        for c in south:
            c.start()

    for c in sides:
        c.start()

    @pl.when(i == 0)
    def _():
        hrow[0] = jnp.zeros((2 * NV, LANES), BF16)
        hcol[2] = jnp.zeros((2 * NV, LANES), BF16)
        hcol[3] = jnp.zeros((2 * NV, LANES), BF16)

    @pl.when(i == NA - 1)
    def _():
        hrow[1] = jnp.zeros((2 * NV, LANES), BF16)
        hcol[4] = jnp.zeros((2 * NV, LANES), BF16)
        hcol[5] = jnp.zeros((2 * NV, LANES), BF16)

    for c in sides:
        c.wait()

    @pl.when(i > 0)
    def _():
        for c in north:
            c.wait_recv()

    @pl.when(i < NA - 1)
    def _():
        for c in north:
            c.wait_send()
        for c in south:
            c.wait_recv()

    @pl.when(i > 0)
    def _():
        for c in south:
            c.wait_send()


def kernel(
    xv, cw, cb, ow, oi, oc, ov, og, hcol_s, hrow, hcol, out_ref,
    big, s1, s2, wt, owt,
    fc, recv, back, res, pick_s, hx, gsend, grecv, ep, oh, sp, ets, hs, kr, fr, ob, obs_s, obs_r,
    asend, arecv, psend, precv, gsend_sem, grecv_sem, bsend, brecv, osem,
):
    k, i, j, peer = place()
    i2 = lax.rem(i + 2, NA)
    k_hi, k_y, k_c = lax.div(k, 16), lax.rem(lax.div(k, 2), 8), lax.rem(k, 2)

    def partner(s):
        s = lax.rem(s + 1, NE)
        u = lax.div(s, 4)
        dy = lax.div(u + 1, 2) * (2 * lax.rem(u, 2) - 1)
        hi = lax.rem(k_hi + s, 2)
        y = lax.rem(k_y + 8 + dy, 8)
        c = lax.rem(k_c + lax.div(s, 2), 2)
        return hi * 16 + y * 2 + c

    met = meet(
        [peer(0, di, dj) for di in range(NA) for dj in range(NB) if di or dj]
        + [peer(dk, di, 0) for dk in range(1, NE) for di in (0, 2)]
    )
    lane24 = lane_iota((NV, LANES))
    fill(big, xv)

    def row_of(r):
        return big[pl.ds(r, NV, stride=PITCH), :]

    def over(n, body):
        lax.fori_loop(0, n, lambda s, c: (body(s), c)[1], 0)

    def each(start, stop, body):
        for s in range(start, stop):
            body(toward(s))

    def toward(s):
        s = (s + 1) % NE
        u = s // 4
        dy = ((u + 1) // 2) * (2 * (u % 2) - 1)
        hi = 1 - k_hi if s % 2 else k_hi
        y = lax.rem(k_y + (8 + dy) % 8, 8)
        c = 1 - k_c if (s // 2) % 2 else k_c
        return hi * 16 + y * 2 + c

    w = cw[...].astype(F32)
    b = cb[...]
    b_hi = b.astype(BF16).astype(F32)
    b_mid = (b - b_hi).astype(BF16).astype(F32)
    b_lo = b - b_hi - b_mid
    zeros8 = jnp.zeros((8, 256), F32)
    pad = row_iota((8, 256))
    bias8 = jnp.where(pad == 0, b_hi, jnp.where(pad == 1, b_mid, jnp.where(pad == 2, b_lo, zeros8)))
    wfull = jnp.concatenate(
        [w[0:72], bias8, w[72:144], zeros8, w[144:216], zeros8, zeros8, zeros8], axis=0
    )
    wt[...] = wfull.T.astype(BF16)
    owp = ow[...].astype(F32) * 0.5
    owt[...] = jnp.concatenate([owp, jnp.zeros((8, 256), F32)], axis=0).astype(BF16)
    tail = jnp.zeros((16, LANES), BF16)
    s1[68 * SLAB : 68 * SLAB + 16, :] = tail
    s2[66 * SLAB : 66 * SLAB + 16, :] = tail

    def pair(ref, n):
        both = ref[n].astype(F32)
        return both[0:NV], both[NV : 2 * NV]

    n0, n1 = pair(hrow, 0)
    m0, m1 = pair(hrow, 1)

    def ext(mid, top, bottom):
        out = roll(mid, 2)
        out = jnp.where(lane24 < 2, roll(top, 2 - ROWS), out)
        return jnp.where(lane24 > ROWS + 1, roll(bottom, ROWS + 2), out)

    w_m, w_n, w_s = pair(hcol, 0), pair(hcol, 2), pair(hcol, 4)
    e_m, e_n, e_s = pair(hcol, 1), pair(hcol, 3), pair(hcol, 5)
    cm2 = ext(w_m[0], w_n[0], w_s[0])
    cm1 = ext(w_m[1], w_n[1], w_s[1])
    cp0 = ext(e_m[0], e_n[0], e_s[0])
    cp1 = ext(e_m[1], e_n[1], e_s[1])

    def own(mid, lane):
        out = roll(mid, 2)
        for at, x in ((0, n0), (1, n1), (ROWS + 2, m0), (ROWS + 3, m1)):
            out = jnp.where(lane24 == at, roll(x, at - lane), out)
        return out

    c0e = own(pair(hcol_s, 0)[0], 0)
    c127e = own(pair(hcol_s, 1)[1], LANES - 1)

    def put1(n, x):
        s1[n * SLAB : (n + 1) * SLAB, :] = slab(x, roll(cm1, -n), roll(cp0, LANES - 1 - n))

    for n, x in ((0, n0), (1, n1), (ROWS + 2, m0), (ROWS + 3, m1)):
        put1(n, x)

    for row in range(ROWS):
        put1(row + 2, row_of(row))

    weights = wt[...]
    oweights = owt[...]

    def edge(a0, a1, a2):
        ones = jnp.ones((8, LANES), F32)
        rows = []
        for a in range(3):
            rows += [roll(a0, -a), roll(a1, -a), roll(a2, -a), ones]
        rows.append(jnp.zeros((16, LANES), F32))
        return jnp.concatenate(rows, axis=0).astype(BF16)

    first, last = i > 0, i < NA - 1
    ep[:, 0:LANES] = edge(cm2, cm1, c0e)
    ep[:, LANES : 2 * LANES] = edge(c127e, cp0, cp1)
    ch = changes(weights, oweights, ep[...])
    inside = ((lane24 > 0) | first) & ((lane24 < ROWS + 1) | last)
    mw = jnp.where(inside, roll(cm1, -1) + ch[0:NV, 0:LANES], 0.0)
    me = jnp.where(inside, roll(cp0, -1) + ch[0:NV, LANES : 2 * LANES], 0.0)

    def hide(s, n, q):
        base = pl.multiple_of(n * SLAB, 16)
        p = jnp.concatenate([s[pl.ds(base, 256), :], s[pl.ds(base + SLAB, 256), :]], axis=1)
        hs[q] = gelu2(dot(wt[...], p))

    def tile(s, n, q):
        base = pl.multiple_of(n * SLAB, 16)
        c = dot(owt[...], hs[q])
        mid0 = s[pl.ds(base + SLAB, SLAB), :].astype(F32)[NV : 2 * NV]
        mid1 = s[pl.ds(base + 2 * SLAB, SLAB), :].astype(F32)[NV : 2 * NV]
        return mid0 + c[0:NV, 0:LANES], mid1 + c[0:NV, LANES : 2 * LANES]

    def step1(outer, carry):
        for q in range(11):
            hide(s1, (outer * 11 + q) * 2, q)
        for q in range(11):
            n = (outer * 11 + q) * 2
            for d, m in enumerate(tile(s1, n, q)):
                at = n + d
                keep = ((at > 0) | first) & ((at < ROWS + 1) | last)
                m = jnp.where(keep, m, 0.0)
                s2[pl.ds(pl.multiple_of(at * SLAB, 16), SLAB), :] = slab(
                    m,
                    roll(mw, (LANES - at) % LANES),
                    roll(me, (2 * LANES - 1 - at) % LANES),
                )
        return carry

    lax.fori_loop(0, 3, step1, 0)

    live = (lane_iota((1, NOBS)) < oc[...]).astype(F32)
    obs_s[0:1, :] = ov[0]
    obs_s[1:2, :] = og[0] * live
    obs_s[2:8, :] = jnp.zeros((6, NOBS), F32)

    flat = oi[0]
    v_of, r_of, c_of = flat // 8192, (flat // LANES) % ROWS, flat % LANES
    oh[...] = marks(row_iota((LANES, NOBS)) == c_of)

    def columns(outer):
        rows = pl.ds(pl.multiple_of(outer * (22 * SLAB), 16), 22 * SLAB)
        ob[rows, :] = dot(s2[rows, :], oh[...]).astype(BF16)

    over(3, columns)

    def gather(outer, taps):
        for q in range(11):
            n = outer * 11 + q
            part = ob[pl.ds(pl.multiple_of(n * SLAB, 16), SLAB), :]
            taps = tuple(t + part * marks(r_of == n - a) for a, t in enumerate(taps))
        return taps

    taps = lax.fori_loop(0, 6, gather, (jnp.zeros((SLAB, NOBS), BF16),) * 3)
    for a in range(3):
        ep[a * SLAB : (a + 1) * SLAB, :] = taps[a]
    ep[3 * SLAB : 256, :] = jnp.zeros((16, NOBS), BF16)
    seen = taps[1].astype(F32)[NV : 2 * NV] + changes(weights, oweights, ep[...])[0:NV]
    seen = seen.astype(BF16).astype(F32)
    pick_s[0] = jnp.sum(jnp.where(row_iota((NV, NOBS)) == v_of, seen, 0.0), axis=0, keepdims=True)

    def send_pick(t):
        return pltpu.make_async_remote_copy(
            src_ref=pick_s.at[0], dst_ref=hx.at[k], send_sem=psend.at[t], recv_sem=precv.at[k],
            device_id=(t, i2, j), device_id_type=MESH,
        )

    def send_tile(t):
        return pltpu.make_async_remote_copy(
            src_ref=fc.at[t], dst_ref=recv.at[k], send_sem=asend.at[t], recv_sem=arecv.at[k],
            device_id=(t, i, j), device_id_type=MESH,
        )

    def step2(outer, carry):
        for q in range(8):
            hide(s2, partner(outer * 8 + q) * 2, q)
        for q in range(8):
            s = outer * 8 + q
            t = partner(s)
            f0, f1 = tile(s2, t * 2, q)
            fc[t] = jnp.concatenate([f0, f1], axis=0).astype(BF16)
        return carry

    obs_copy = pltpu.make_async_remote_copy(
        src_ref=obs_s, dst_ref=obs_r, send_sem=osem.at[0], recv_sem=osem.at[1],
        device_id=(k, i2, j), device_id_type=MESH,
    )
    met()
    each(0, NE, lambda t: send_pick(t).start())
    obs_copy.start()
    lax.fori_loop(0, 1, step2, 0)
    each(0, 8, lambda t: send_tile(t).start())
    lax.fori_loop(1, 4, step2, 0)

    def recv_pick(t):
        return pltpu.make_async_remote_copy(
            src_ref=pick_s.at[0], dst_ref=hx.at[t], send_sem=psend.at[t], recv_sem=precv.at[t],
            device_id=(t, i2, j), device_id_type=MESH,
        )

    over(NE, lambda t: recv_pick(t).wait_recv())

    values = hx[:, 0, :]
    obs_copy.wait()
    value = obs_r[0:1, :]
    weight = obs_r[1:2, :]
    mean = jnp.mean(values, axis=0, keepdims=True)
    dev = values - mean
    innov = value - mean
    rows40 = jnp.concatenate([dev, jnp.broadcast_to(innov, (8, NOBS))], axis=0)
    wdev = dev * weight
    hp = lax.Precision.HIGHEST
    g4 = dot(rows40, jnp.concatenate([wdev] * 4, axis=0), ((1,), (1,)), hp)
    lane8 = lane_iota((8, LANES))
    packed = jnp.zeros((8, LANES), F32)
    for q in range(4):
        packed = jnp.where(lane8 // 32 == q, g4[8 * q : 8 * q + 8], packed)
    row8 = row_iota((8, LANES))
    spare = (
        ((row8 == 0) & (lane8 > 1) & (lane8 < NE))
        | ((row8 == 1) & (lane8 == 0))
        | ((row8 == 2) & (lane8 == 1))
    )
    mine = jnp.where(spare, g4[32:40], packed)
    gsend[...] = mine
    slot = i * NB + j
    grecv[slot] = mine

    def send_gram(di, dj):
        n = (di % NA) * NB + dj % NB
        return pltpu.make_async_remote_copy(
            src_ref=gsend, dst_ref=grecv.at[slot], send_sem=gsend_sem.at[n],
            recv_sem=grecv_sem.at[slot], device_id=peer(0, di, dj), device_id_type=MESH,
        )

    def recv_gram(di, dj):
        n = ((i + di) % NA) * NB + (j + dj) % NB
        return pltpu.make_async_remote_copy(
            src_ref=gsend, dst_ref=grecv.at[n], send_sem=gsend_sem.at[0],
            recv_sem=grecv_sem.at[n], device_id=peer(0, di, dj), device_id_type=MESH,
        )

    others = [(di, dj) for di in range(NA) for dj in range(NB) if di or dj]
    for di, dj in others:
        send_gram(di, dj).start()
    each(8, NE - 1, lambda t: send_tile(t).start())
    for di, dj in others:
        recv_gram(di, dj).wait_recv()

    total = grecv[0]
    for n in range(1, NA * NB):
        total = total + grecv[n]
    square = jnp.concatenate([roll(total, -32 * q)[:, 0:NE] for q in range(4)], axis=0)
    row32, lane32 = row_iota((NE, NE)), lane_iota((NE, NE))
    taken = (
        ((row32 == 0) & (lane32 > 1))
        | ((row32 == 1) & (lane32 == 0))
        | ((row32 == 2) & (lane32 == 1))
    )
    gram = jnp.where(taken, square.T, square)
    lane1 = lane_iota((1, NE))
    proj = jnp.where(lane1 == 0, square[1:2], jnp.where(lane1 == 1, square[2:3], square[0:1]))
    proj = jnp.broadcast_to(proj, (8, NE))
    eye = jnp.where(row_iota((NE, NE)) == lane_iota((NE, NE)), 1.0, 0.0)
    system = (NE - 1) * eye + gram

    def full_sum(a):
        return jnp.sum(jnp.sum(a, axis=1, keepdims=True), axis=0, keepdims=True)

    scale = jnp.sqrt(full_sum(system * system))

    current = system / scale
    inverse = 1.5 * eye - 0.5 * current
    current = dot(current, inverse, precision=hp)
    for _ in range(NS_ITERS - 1):
        factor = 1.5 * eye - 0.5 * dot(inverse, current, precision=hp)
        current, inverse = dot(current, factor, precision=hp), dot(factor, inverse, precision=hp)
    root = inverse / jnp.sqrt(scale)
    half = dot(proj, root, precision=hp)
    mean_w = dot(half, root, precision=hp)[0:1]
    full = mean_w + math.sqrt(NE - 1.0) * root
    et = 1.0 / NE + full - jnp.mean(full, axis=1, keepdims=True)
    et_hi = et.astype(BF16)
    et_lo = (et - et_hi.astype(F32)).astype(BF16)

    spread = marks(row_iota((512, NE)) // 16 == lane_iota((512, NE)))
    sp[...] = marks(row_iota((NE, 512)) == lane_iota((NE, 512)) // 16)
    ets[0] = et_hi
    ets[1] = et_lo
    same = row_iota((512, 512)) % 16 == lane_iota((512, 512)) % 16

    def kron(e):
        a = dot(spread, e).astype(BF16)
        return jnp.where(same, dot(a, sp[...]), 0.0).astype(BF16)

    kr[0] = kron(ets[0])
    kr[1] = kron(ets[1])

    def recv_tile(t):
        return pltpu.make_async_remote_copy(
            src_ref=fc.at[t], dst_ref=recv.at[t], send_sem=asend.at[t], recv_sem=arecv.at[t],
            device_id=(t, i, j), device_id_type=MESH,
        )

    recv[k] = fc[k]
    each(0, NE - 1, lambda t: recv_tile(t).wait_recv())

    for q in range(3):
        fr[:, q * LANES : (q + 1) * LANES] = recv[:, 16 * q : 16 * q + 16, :].reshape(512, LANES)

    def send_back(t):
        return pltpu.make_async_remote_copy(
            src_ref=back.at[t], dst_ref=res.at[k], send_sem=bsend.at[t], recv_sem=brecv.at[k],
            device_id=(t, i, j), device_id_type=MESH,
        )

    def recv_back(t):
        return pltpu.make_async_remote_copy(
            src_ref=back.at[t], dst_ref=res.at[t], send_sem=bsend.at[t], recv_sem=brecv.at[t],
            device_id=(t, i, j), device_id_type=MESH,
        )

    def group(g):
        return lax.rem(lax.div(k, 8) + 1 + g, 4)

    def send_group(g):
        for e in range(8 if g < 3 else 7):
            send_back(group(g) * 8 + lax.rem(k + 1 + e, 8)).start()

    for g in range(4):
        rows = pl.ds(pl.multiple_of(group(g) * LANES, LANES), LANES)
        o = (dot(kr[0, rows, :], fr[...]) + dot(kr[1, rows, :], fr[...])).astype(BF16)
        for q in range(3):
            back[pl.ds(group(g) * 8, 8), 16 * q : 16 * q + 16, :] = o[
                :, q * LANES : (q + 1) * LANES
            ].reshape(8, 16, LANES)
        if g:
            send_group(g - 1)
    send_group(3)
    res[k] = back[k]

    def finish(s):
        t = partner(s)

        @pl.when(s < NE - 1)
        def _():
            recv_back(t).wait_recv()

        big[pl.ds(pl.multiple_of(t * 48, 16), 48), :] = res[t].astype(F32)

    over(NE, finish)
    for v in range(NV):
        out_ref[0, v] = big[pl.ds(v, ROWS, stride=NV), :].astype(BF16)

    over(NE, lambda t: recv_pick(t).wait_send())
    over(NE - 1, lambda s: recv_tile(partner(s)).wait_send())
    over(NE - 1, lambda s: recv_back(partner(s)).wait_send())
    for di, dj in others:
        send_gram(di, dj).wait_send()


def per_device(x, cw, cb, ow, oi, oc, ov, og):
    vmem = pl.BlockSpec(memory_space=pltpu.VMEM)
    hcol_s, hrow, hcol = pl.pallas_call(
        halo_kernel,
        out_shape=(
            jax.ShapeDtypeStruct((2, 2 * NV, LANES), BF16),
            jax.ShapeDtypeStruct((2, 2 * NV, LANES), BF16),
            jax.ShapeDtypeStruct((6, 2 * NV, LANES), BF16),
        ),
        in_specs=[pl.BlockSpec(memory_space=pl.ANY)],
        out_specs=(vmem,) * 3,
        scratch_shapes=[
            pltpu.VMEM(x.shape, BF16),
            pltpu.VMEM((NV * PITCH, LANES), F32),
            pltpu.VMEM((2, 2 * NV, LANES), BF16),
            pltpu.SemaphoreType.DMA,
            pltpu.SemaphoreType.DMA((9,)),
            pltpu.SemaphoreType.DMA((9,)),
        ],
        compiler_params=pltpu.CompilerParams(
            collective_id=0, has_side_effects=True, vmem_limit_bytes=16 * 1024 * 1024
        ),
        cost_estimate=pl.CostEstimate(flops=10**10, bytes_accessed=10**6, transcendentals=0),
        name="halo",
    )(x)
    return pl.pallas_call(
        kernel,
        out_shape=jax.ShapeDtypeStruct(x.shape, x.dtype),
        in_specs=[vmem] * 11,
        out_specs=vmem,
        scratch_shapes=[
            pltpu.VMEM((NV * PITCH, LANES), F32),
            pltpu.VMEM((68 * SLAB + 16, LANES), BF16),
            pltpu.VMEM((66 * SLAB + 16, LANES), BF16),
            pltpu.VMEM((256, 256), BF16),
            pltpu.VMEM((32, 256), BF16),
            pltpu.VMEM((NE, 2 * NV, LANES), BF16),
            pltpu.VMEM((NE, 2 * NV, LANES), BF16),
            pltpu.VMEM((NE, 2 * NV, LANES), BF16),
            pltpu.VMEM((NE, 2 * NV, LANES), BF16),
            pltpu.VMEM((1, 1, NOBS), F32),
            pltpu.VMEM((NE, 1, NOBS), F32),
            pltpu.VMEM((8, LANES), F32),
            pltpu.VMEM((NA * NB, 8, LANES), F32),
            pltpu.VMEM((256, 256), BF16),
            pltpu.VMEM((LANES, NOBS), BF16),
            pltpu.VMEM((NE, 512), BF16),
            pltpu.VMEM((2, NE, NE), BF16),
            pltpu.VMEM((11, 256, 256), BF16),
            pltpu.VMEM((2, 512, 512), BF16),
            pltpu.VMEM((512, 3 * LANES), BF16),
            pltpu.VMEM((66 * SLAB, NOBS), BF16),
            pltpu.VMEM((8, NOBS), F32),
            pltpu.VMEM((8, NOBS), F32),
            pltpu.SemaphoreType.DMA((NE,)),
            pltpu.SemaphoreType.DMA((NE,)),
            pltpu.SemaphoreType.DMA((NE,)),
            pltpu.SemaphoreType.DMA((NE,)),
            pltpu.SemaphoreType.DMA((NA * NB,)),
            pltpu.SemaphoreType.DMA((NA * NB,)),
            pltpu.SemaphoreType.DMA((NE,)),
            pltpu.SemaphoreType.DMA((NE,)),
            pltpu.SemaphoreType.DMA((2,)),
        ],
        compiler_params=pltpu.CompilerParams(
            collective_id=1, has_side_effects=True, vmem_limit_bytes=32 * 1024 * 1024
        ),
        name="cycle",
    )(x, cw, cb.reshape(1, 256), ow.T, oi, oc, ov, og, hcol_s, hrow, hcol)


def solution(mesh):
    return jax.shard_map(
        per_device,
        mesh=mesh,
        in_specs=(
            P("ens", None, "lat", "lon"),
            P(),
            P(),
            P(),
            P("lat", "lon", None),
            P("lat", "lon"),
            P("lat", "lon", None),
            P("lat", "lon", None),
        ),
        out_specs=P("ens", None, "lat", "lon"),
        check_vma=False,
    )
```

```python
import math

import jax
import jax.numpy as jnp
from jax import lax
from jax.experimental import pallas as pl
from jax.experimental.pallas import tpu as pltpu
from jax.sharding import PartitionSpec as P

NS_ITERS = 20
MESH = pl.DeviceIdType.MESH
F32 = jnp.float32
BF16 = jnp.bfloat16
NV = 24
ROWS = 64
LANES = 128
SLAB = 80
NE = 32
NA = 4
NB = 4
PITCH = 72
NOBS = 256


def dot(a, b, dims=((1,), (0,)), precision=None):
    return lax.dot_general(
        a, b, (dims, ((), ())), precision=precision, preferred_element_type=F32
    )


def marks(hit):
    return jnp.where(hit, 1.0, 0.0).astype(BF16)


def lane_iota(shape):
    return lax.broadcasted_iota(jnp.int32, shape, len(shape) - 1)


def row_iota(shape):
    return lax.broadcasted_iota(jnp.int32, shape, len(shape) - 2)


def roll(x, shift):
    if isinstance(shift, int):
        shift = shift % LANES
        if shift == 0:
            return x
    return pltpu.roll(x, shift, 1)


def slab(x, west, east):
    lane = lane_iota((NV, LANES))
    xw = jnp.where(lane == 0, west, roll(x, 1))
    xe = jnp.where(lane == LANES - 1, east, roll(x, -1))
    return jnp.concatenate([xw, x, xe, jnp.ones((8, LANES), F32)], axis=0).astype(BF16)


def gelu2(pre):
    c1 = math.sqrt(2.0 / math.pi)
    c2 = c1 * 0.044715
    x = pre.astype(BF16)
    th = jnp.tanh(x * (jnp.bfloat16(c1) + jnp.bfloat16(c2) * (x * x)))
    return x + x * th


def changes(wt, ow, patches):
    pre = dot(wt, patches)
    return dot(ow, gelu2(pre))


def fill(big, xv):
    for v in range(NV):
        big[v * PITCH : v * PITCH + ROWS, :] = xv[0, v].astype(F32)


def place():
    k = lax.axis_index("ens")
    i = lax.axis_index("lat")
    j = lax.axis_index("lon")

    def peer(dk, di, dj):
        return tuple(
            at if d % n == 0 else lax.rem(at + d % n, n)
            for at, d, n in ((k, dk, NE), (i, di, NA), (j, dj, NB))
        )

    return k, i, j, peer


def meet(peers):
    barrier = pltpu.get_barrier_semaphore()
    for to in peers:
        pl.semaphore_signal(barrier, inc=1, device_id=to, device_id_type=MESH)
    return lambda: pl.semaphore_wait(barrier, len(peers))


def halo_kernel(
    x_hbm, hcol_s, hrow, hcol,
    xv, big, hrow_s, load_sem, hsend, hrecv,
):
    k, i, j, peer = place()
    load = pltpu.make_async_copy(x_hbm, xv, load_sem)
    load.start()
    met = meet(
        [peer(0, di, dj) for di in (0, 1, -1) for dj in (0, 1, -1) if di or dj]
    )
    load.wait()
    lane24 = lane_iota((NV, LANES))

    fill(big, xv)

    def row_of(r):
        return big[pl.ds(r, NV, stride=PITCH), :]

    zero24 = jnp.zeros((NV, LANES), F32)
    cols = (zero24,) * 4
    for row in range(ROWS):
        x = roll(row_of(row), row)
        cols = tuple(
            jnp.where(lane24 == (row + off) % LANES, x, c)
            for c, off in zip(cols, (0, 1, LANES - 2, LANES - 1))
        )
    c0, c1, c126, c127 = cols
    c1 = roll(c1, -1)
    c126 = roll(c126, 2)
    c127 = roll(c127, 1)
    hcol_s[0] = jnp.concatenate([c0, c1], axis=0).astype(BF16)
    hcol_s[1] = jnp.concatenate([c126, c127], axis=0).astype(BF16)
    hrow_s[0] = jnp.concatenate([row_of(0), row_of(1)], axis=0).astype(BF16)
    hrow_s[1] = jnp.concatenate([row_of(ROWS - 2), row_of(ROWS - 1)], axis=0).astype(BF16)
    met()

    def halo(src, dst, n, di, dj):
        return pltpu.make_async_remote_copy(
            src_ref=src, dst_ref=dst, send_sem=hsend.at[n], recv_sem=hrecv.at[n],
            device_id=peer(0, di, dj), device_id_type=MESH,
        )

    north = [
        halo(hrow_s.at[1], hrow.at[0], 0, 1, 0),
        halo(hcol_s.at[1], hcol.at[2], 4, 1, 1),
        halo(hcol_s.at[0], hcol.at[3], 5, 1, -1),
    ]
    south = [
        halo(hrow_s.at[0], hrow.at[1], 1, -1, 0),
        halo(hcol_s.at[1], hcol.at[4], 6, -1, 1),
        halo(hcol_s.at[0], hcol.at[5], 7, -1, -1),
    ]
    sides = [
        halo(hcol_s.at[1], hcol.at[0], 2, 0, 1),
        halo(hcol_s.at[0], hcol.at[1], 3, 0, -1),
    ]

    @pl.when(i < NA - 1)
    def _():
        for c in north:
            c.start()

    @pl.when(i > 0)
    def _():
        for c in south:
            c.start()

    for c in sides:
        c.start()

    @pl.when(i == 0)
    def _():
        hrow[0] = jnp.zeros((2 * NV, LANES), BF16)
        hcol[2] = jnp.zeros((2 * NV, LANES), BF16)
        hcol[3] = jnp.zeros((2 * NV, LANES), BF16)

    @pl.when(i == NA - 1)
    def _():
        hrow[1] = jnp.zeros((2 * NV, LANES), BF16)
        hcol[4] = jnp.zeros((2 * NV, LANES), BF16)
        hcol[5] = jnp.zeros((2 * NV, LANES), BF16)

    for c in sides:
        c.wait()

    @pl.when(i > 0)
    def _():
        for c in north:
            c.wait_recv()

    @pl.when(i < NA - 1)
    def _():
        for c in north:
            c.wait_send()
        for c in south:
            c.wait_recv()

    @pl.when(i > 0)
    def _():
        for c in south:
            c.wait_send()


def kernel(
    xv, cw, cb, ow, oi, oc, ov, og, hcol_s, hrow, hcol, out_ref,
    big, s1, s2, wt, owt,
    fc, recv, back, res, pick_s, hx, gsend, grecv, ep, oh, sp, ets, hs, kr, fr, ob, obs_s, obs_r,
    asend, arecv, psend, precv, gsend_sem, grecv_sem, bsend, brecv, osem,
):
    k, i, j, peer = place()
    i2 = lax.rem(i + 2, NA)
    k_hi, k_y, k_c = lax.div(k, 16), lax.rem(lax.div(k, 2), 8), lax.rem(k, 2)

    def partner(s):
        s = lax.rem(s + 1, NE)
        u = lax.div(s, 4)
        dy = lax.div(u + 1, 2) * (2 * lax.rem(u, 2) - 1)
        hi = lax.rem(k_hi + s, 2)
        y = lax.rem(k_y + 8 + dy, 8)
        c = lax.rem(k_c + lax.div(s, 2), 2)
        return hi * 16 + y * 2 + c

    met = meet(
        [peer(0, di, dj) for di in range(NA) for dj in range(NB) if di or dj]
        + [peer(dk, di, 0) for dk in range(1, NE) for di in (0, 2)]
    )
    lane24 = lane_iota((NV, LANES))
    fill(big, xv)

    def row_of(r):
        return big[pl.ds(r, NV, stride=PITCH), :]

    def over(n, body):
        lax.fori_loop(0, n, lambda s, c: (body(s), c)[1], 0)

    def each(start, stop, body):
        for s in range(start, stop):
            body(toward(s))

    def toward(s):
        s = (s + 1) % NE
        u = s // 4
        dy = ((u + 1) // 2) * (2 * (u % 2) - 1)
        hi = 1 - k_hi if s % 2 else k_hi
        y = lax.rem(k_y + (8 + dy) % 8, 8)
        c = 1 - k_c if (s // 2) % 2 else k_c
        return hi * 16 + y * 2 + c

    w = cw[...].astype(F32)
    b = cb[...]
    b_hi = b.astype(BF16).astype(F32)
    b_mid = (b - b_hi).astype(BF16).astype(F32)
    b_lo = b - b_hi - b_mid
    zeros8 = jnp.zeros((8, 256), F32)
    pad = row_iota((8, 256))
    bias8 = jnp.where(pad == 0, b_hi, jnp.where(pad == 1, b_mid, jnp.where(pad == 2, b_lo, zeros8)))
    wfull = jnp.concatenate(
        [w[0:72], bias8, w[72:144], zeros8, w[144:216], zeros8, zeros8, zeros8], axis=0
    )
    wt[...] = wfull.T.astype(BF16)
    owp = ow[...].astype(F32) * 0.5
    owt[...] = jnp.concatenate([owp, jnp.zeros((8, 256), F32)], axis=0).astype(BF16)
    tail = jnp.zeros((16, LANES), BF16)
    s1[68 * SLAB : 68 * SLAB + 16, :] = tail
    s2[66 * SLAB : 66 * SLAB + 16, :] = tail

    def pair(ref, n):
        both = ref[n].astype(F32)
        return both[0:NV], both[NV : 2 * NV]

    n0, n1 = pair(hrow, 0)
    m0, m1 = pair(hrow, 1)

    def ext(mid, top, bottom):
        out = roll(mid, 2)
        out = jnp.where(lane24 < 2, roll(top, 2 - ROWS), out)
        return jnp.where(lane24 > ROWS + 1, roll(bottom, ROWS + 2), out)

    w_m, w_n, w_s = pair(hcol, 0), pair(hcol, 2), pair(hcol, 4)
    e_m, e_n, e_s = pair(hcol, 1), pair(hcol, 3), pair(hcol, 5)
    cm2 = ext(w_m[0], w_n[0], w_s[0])
    cm1 = ext(w_m[1], w_n[1], w_s[1])
    cp0 = ext(e_m[0], e_n[0], e_s[0])
    cp1 = ext(e_m[1], e_n[1], e_s[1])

    def own(mid, lane):
        out = roll(mid, 2)
        for at, x in ((0, n0), (1, n1), (ROWS + 2, m0), (ROWS + 3, m1)):
            out = jnp.where(lane24 == at, roll(x, at - lane), out)
        return out

    c0e = own(pair(hcol_s, 0)[0], 0)
    c127e = own(pair(hcol_s, 1)[1], LANES - 1)

    def put1(n, x):
        s1[n * SLAB : (n + 1) * SLAB, :] = slab(x, roll(cm1, -n), roll(cp0, LANES - 1 - n))

    for n, x in ((0, n0), (1, n1), (ROWS + 2, m0), (ROWS + 3, m1)):
        put1(n, x)

    for row in range(ROWS):
        put1(row + 2, row_of(row))

    weights = wt[...]
    oweights = owt[...]

    def edge(a0, a1, a2):
        ones = jnp.ones((8, LANES), F32)
        rows = []
        for a in range(3):
            rows += [roll(a0, -a), roll(a1, -a), roll(a2, -a), ones]
        rows.append(jnp.zeros((16, LANES), F32))
        return jnp.concatenate(rows, axis=0).astype(BF16)

    first, last = i > 0, i < NA - 1
    ep[:, 0:LANES] = edge(cm2, cm1, c0e)
    ep[:, LANES : 2 * LANES] = edge(c127e, cp0, cp1)
    ch = changes(weights, oweights, ep[...])
    inside = ((lane24 > 0) | first) & ((lane24 < ROWS + 1) | last)
    mw = jnp.where(inside, roll(cm1, -1) + ch[0:NV, 0:LANES], 0.0)
    me = jnp.where(inside, roll(cp0, -1) + ch[0:NV, LANES : 2 * LANES], 0.0)

    def hide(s, n, q):
        base = pl.multiple_of(n * SLAB, 16)
        p = jnp.concatenate([s[pl.ds(base, 256), :], s[pl.ds(base + SLAB, 256), :]], axis=1)
        hs[q] = gelu2(dot(wt[...], p))

    def tile(s, n, q):
        base = pl.multiple_of(n * SLAB, 16)
        c = dot(owt[...], hs[q])
        mid0 = s[pl.ds(base + SLAB, SLAB), :].astype(F32)[NV : 2 * NV]
        mid1 = s[pl.ds(base + 2 * SLAB, SLAB), :].astype(F32)[NV : 2 * NV]
        return mid0 + c[0:NV, 0:LANES], mid1 + c[0:NV, LANES : 2 * LANES]

    def step1(outer, carry):
        for q in range(11):
            hide(s1, (outer * 11 + q) * 2, q)
        for q in range(11):
            n = (outer * 11 + q) * 2
            for d, m in enumerate(tile(s1, n, q)):
                at = n + d
                keep = ((at > 0) | first) & ((at < ROWS + 1) | last)
                m = jnp.where(keep, m, 0.0)
                s2[pl.ds(pl.multiple_of(at * SLAB, 16), SLAB), :] = slab(
                    m,
                    roll(mw, (LANES - at) % LANES),
                    roll(me, (2 * LANES - 1 - at) % LANES),
                )
        return carry

    lax.fori_loop(0, 3, step1, 0)

    live = (lane_iota((1, NOBS)) < oc[...]).astype(F32)
    obs_s[0:1, :] = ov[0]
    obs_s[1:2, :] = og[0] * live
    obs_s[2:8, :] = jnp.zeros((6, NOBS), F32)

    flat = oi[0]
    v_of, r_of, c_of = flat // 8192, (flat // LANES) % ROWS, flat % LANES
    oh[...] = marks(row_iota((LANES, NOBS)) == c_of)

    def columns(outer):
        rows = pl.ds(pl.multiple_of(outer * (22 * SLAB), 16), 22 * SLAB)
        ob[rows, :] = dot(s2[rows, :], oh[...]).astype(BF16)

    over(3, columns)

    def gather(outer, taps):
        for q in range(11):
            n = outer * 11 + q
            part = ob[pl.ds(pl.multiple_of(n * SLAB, 16), SLAB), :]
            taps = tuple(t + part * marks(r_of == n - a) for a, t in enumerate(taps))
        return taps

    taps = lax.fori_loop(0, 6, gather, (jnp.zeros((SLAB, NOBS), BF16),) * 3)
    for a in range(3):
        ep[a * SLAB : (a + 1) * SLAB, :] = taps[a]
    ep[3 * SLAB : 256, :] = jnp.zeros((16, NOBS), BF16)
    seen = taps[1].astype(F32)[NV : 2 * NV] + changes(weights, oweights, ep[...])[0:NV]
    seen = seen.astype(BF16).astype(F32)
    pick_s[0] = jnp.sum(jnp.where(row_iota((NV, NOBS)) == v_of, seen, 0.0), axis=0, keepdims=True)

    def send_pick(t):
        return pltpu.make_async_remote_copy(
            src_ref=pick_s.at[0], dst_ref=hx.at[k], send_sem=psend.at[t], recv_sem=precv.at[k],
            device_id=(t, i2, j), device_id_type=MESH,
        )

    def send_tile(t):
        return pltpu.make_async_remote_copy(
            src_ref=fc.at[t], dst_ref=recv.at[k], send_sem=asend.at[t], recv_sem=arecv.at[k],
            device_id=(t, i, j), device_id_type=MESH,
        )

    def step2(outer, carry):
        for q in range(8):
            hide(s2, partner(outer * 8 + q) * 2, q)
        for q in range(8):
            s = outer * 8 + q
            t = partner(s)
            f0, f1 = tile(s2, t * 2, q)
            fc[t] = jnp.concatenate([f0, f1], axis=0).astype(BF16)
        return carry

    obs_copy = pltpu.make_async_remote_copy(
        src_ref=obs_s, dst_ref=obs_r, send_sem=osem.at[0], recv_sem=osem.at[1],
        device_id=(k, i2, j), device_id_type=MESH,
    )
    met()
    each(0, NE, lambda t: send_pick(t).start())
    obs_copy.start()
    lax.fori_loop(0, 1, step2, 0)
    each(0, 8, lambda t: send_tile(t).start())
    lax.fori_loop(1, 4, step2, 0)

    def recv_pick(t):
        return pltpu.make_async_remote_copy(
            src_ref=pick_s.at[0], dst_ref=hx.at[t], send_sem=psend.at[t], recv_sem=precv.at[t],
            device_id=(t, i2, j), device_id_type=MESH,
        )

    over(NE, lambda t: recv_pick(t).wait_recv())

    values = hx[:, 0, :]
    obs_copy.wait()
    value = obs_r[0:1, :]
    weight = obs_r[1:2, :]
    mean = jnp.mean(values, axis=0, keepdims=True)
    dev = values - mean
    innov = value - mean
    rows40 = jnp.concatenate([dev, jnp.broadcast_to(innov, (8, NOBS))], axis=0)
    wdev = dev * weight
    hp = lax.Precision.HIGHEST
    g4 = dot(rows40, jnp.concatenate([wdev] * 4, axis=0), ((1,), (1,)), hp)
    lane8 = lane_iota((8, LANES))
    packed = jnp.zeros((8, LANES), F32)
    for q in range(4):
        packed = jnp.where(lane8 // 32 == q, g4[8 * q : 8 * q + 8], packed)
    row8 = row_iota((8, LANES))
    spare = (
        ((row8 == 0) & (lane8 > 1) & (lane8 < NE))
        | ((row8 == 1) & (lane8 == 0))
        | ((row8 == 2) & (lane8 == 1))
    )
    mine = jnp.where(spare, g4[32:40], packed)
    gsend[...] = mine
    slot = i * NB + j
    grecv[slot] = mine

    def send_gram(di, dj):
        n = (di % NA) * NB + dj % NB
        return pltpu.make_async_remote_copy(
            src_ref=gsend, dst_ref=grecv.at[slot], send_sem=gsend_sem.at[n],
            recv_sem=grecv_sem.at[slot], device_id=peer(0, di, dj), device_id_type=MESH,
        )

    def recv_gram(di, dj):
        n = ((i + di) % NA) * NB + (j + dj) % NB
        return pltpu.make_async_remote_copy(
            src_ref=gsend, dst_ref=grecv.at[n], send_sem=gsend_sem.at[0],
            recv_sem=grecv_sem.at[n], device_id=peer(0, di, dj), device_id_type=MESH,
        )

    others = [(di, dj) for di in range(NA) for dj in range(NB) if di or dj]
    for di, dj in others:
        send_gram(di, dj).start()
    each(8, NE - 1, lambda t: send_tile(t).start())
    for di, dj in others:
        recv_gram(di, dj).wait_recv()

    total = grecv[0]
    for n in range(1, NA * NB):
        total = total + grecv[n]
    square = jnp.concatenate([roll(total, -32 * q)[:, 0:NE] for q in range(4)], axis=0)
    row32, lane32 = row_iota((NE, NE)), lane_iota((NE, NE))
    taken = (
        ((row32 == 0) & (lane32 > 1))
        | ((row32 == 1) & (lane32 == 0))
        | ((row32 == 2) & (lane32 == 1))
    )
    gram = jnp.where(taken, square.T, square)
    lane1 = lane_iota((1, NE))
    proj = jnp.where(lane1 == 0, square[1:2], jnp.where(lane1 == 1, square[2:3], square[0:1]))
    proj = jnp.broadcast_to(proj, (8, NE))
    eye = jnp.where(row_iota((NE, NE)) == lane_iota((NE, NE)), 1.0, 0.0)
    system = (NE - 1) * eye + gram

    def full_sum(a):
        return jnp.sum(jnp.sum(a, axis=1, keepdims=True), axis=0, keepdims=True)

    scale = jnp.sqrt(full_sum(system * system))

    current = system / scale
    inverse = 1.5 * eye - 0.5 * current
    current = dot(current, inverse, precision=hp)
    for _ in range(NS_ITERS - 1):
        factor = 1.5 * eye - 0.5 * dot(inverse, current, precision=hp)
        current, inverse = dot(current, factor, precision=hp), dot(factor, inverse, precision=hp)
    root = inverse / jnp.sqrt(scale)
    half = dot(proj, root, precision=hp)
    mean_w = dot(half, root, precision=hp)[0:1]
    full = mean_w + math.sqrt(NE - 1.0) * root
    et = 1.0 / NE + full - jnp.mean(full, axis=1, keepdims=True)
    et_hi = et.astype(BF16)
    et_lo = (et - et_hi.astype(F32)).astype(BF16)

    spread = marks(row_iota((512, NE)) // 16 == lane_iota((512, NE)))
    sp[...] = marks(row_iota((NE, 512)) == lane_iota((NE, 512)) // 16)
    ets[0] = et_hi
    ets[1] = et_lo
    same = row_iota((512, 512)) % 16 == lane_iota((512, 512)) % 16

    def kron(e):
        a = dot(spread, e).astype(BF16)
        return jnp.where(same, dot(a, sp[...]), 0.0).astype(BF16)

    kr[0] = kron(ets[0])
    kr[1] = kron(ets[1])

    def recv_tile(t):
        return pltpu.make_async_remote_copy(
            src_ref=fc.at[t], dst_ref=recv.at[t], send_sem=asend.at[t], recv_sem=arecv.at[t],
            device_id=(t, i, j), device_id_type=MESH,
        )

    recv[k] = fc[k]
    each(0, NE - 1, lambda t: recv_tile(t).wait_recv())

    for q in range(3):
        fr[:, q * LANES : (q + 1) * LANES] = recv[:, 16 * q : 16 * q + 16, :].reshape(512, LANES)

    def send_back(t):
        return pltpu.make_async_remote_copy(
            src_ref=back.at[t], dst_ref=res.at[k], send_sem=bsend.at[t], recv_sem=brecv.at[k],
            device_id=(t, i, j), device_id_type=MESH,
        )

    def recv_back(t):
        return pltpu.make_async_remote_copy(
            src_ref=back.at[t], dst_ref=res.at[t], send_sem=bsend.at[t], recv_sem=brecv.at[t],
            device_id=(t, i, j), device_id_type=MESH,
        )

    def group(g):
        return lax.rem(lax.div(k, 8) + 1 + g, 4)

    def send_group(g):
        for e in range(8 if g < 3 else 7):
            send_back(group(g) * 8 + lax.rem(k + 1 + e, 8)).start()

    for g in range(4):
        rows = pl.ds(pl.multiple_of(group(g) * LANES, LANES), LANES)
        o = (dot(kr[0, rows, :], fr[...]) + dot(kr[1, rows, :], fr[...])).astype(BF16)
        for q in range(3):
            back[pl.ds(group(g) * 8, 8), 16 * q : 16 * q + 16, :] = o[
                :, q * LANES : (q + 1) * LANES
            ].reshape(8, 16, LANES)
        if g:
            send_group(g - 1)
    send_group(3)
    res[k] = back[k]

    def finish(s):
        t = partner(s)

        @pl.when(s < NE - 1)
        def _():
            recv_back(t).wait_recv()

        big[pl.ds(pl.multiple_of(t * 48, 16), 48), :] = res[t].astype(F32)

    over(NE, finish)
    for v in range(NV):
        out_ref[0, v] = big[pl.ds(v, ROWS, stride=NV), :].astype(BF16)

    over(NE, lambda t: recv_pick(t).wait_send())
    each(0, NE - 1, lambda t: recv_tile(t).wait_send())
    each(0, NE - 1, lambda t: recv_back(t).wait_send())
    for di, dj in others:
        send_gram(di, dj).wait_send()


def per_device(x, cw, cb, ow, oi, oc, ov, og):
    vmem = pl.BlockSpec(memory_space=pltpu.VMEM)
    hcol_s, hrow, hcol = pl.pallas_call(
        halo_kernel,
        out_shape=(
            jax.ShapeDtypeStruct((2, 2 * NV, LANES), BF16),
            jax.ShapeDtypeStruct((2, 2 * NV, LANES), BF16),
            jax.ShapeDtypeStruct((6, 2 * NV, LANES), BF16),
        ),
        in_specs=[pl.BlockSpec(memory_space=pl.ANY)],
        out_specs=(vmem,) * 3,
        scratch_shapes=[
            pltpu.VMEM(x.shape, BF16),
            pltpu.VMEM((NV * PITCH, LANES), F32),
            pltpu.VMEM((2, 2 * NV, LANES), BF16),
            pltpu.SemaphoreType.DMA,
            pltpu.SemaphoreType.DMA((9,)),
            pltpu.SemaphoreType.DMA((9,)),
        ],
        compiler_params=pltpu.CompilerParams(
            collective_id=0, has_side_effects=True, vmem_limit_bytes=16 * 1024 * 1024
        ),
        cost_estimate=pl.CostEstimate(flops=10**10, bytes_accessed=10**6, transcendentals=0),
        name="halo",
    )(x)
    return pl.pallas_call(
        kernel,
        out_shape=jax.ShapeDtypeStruct(x.shape, x.dtype),
        in_specs=[vmem] * 11,
        out_specs=vmem,
        scratch_shapes=[
            pltpu.VMEM((NV * PITCH, LANES), F32),
            pltpu.VMEM((68 * SLAB + 16, LANES), BF16),
            pltpu.VMEM((66 * SLAB + 16, LANES), BF16),
            pltpu.VMEM((256, 256), BF16),
            pltpu.VMEM((32, 256), BF16),
            pltpu.VMEM((NE, 2 * NV, LANES), BF16),
            pltpu.VMEM((NE, 2 * NV, LANES), BF16),
            pltpu.VMEM((NE, 2 * NV, LANES), BF16),
            pltpu.VMEM((NE, 2 * NV, LANES), BF16),
            pltpu.VMEM((1, 1, NOBS), F32),
            pltpu.VMEM((NE, 1, NOBS), F32),
            pltpu.VMEM((8, LANES), F32),
            pltpu.VMEM((NA * NB, 8, LANES), F32),
            pltpu.VMEM((256, 256), BF16),
            pltpu.VMEM((LANES, NOBS), BF16),
            pltpu.VMEM((NE, 512), BF16),
            pltpu.VMEM((2, NE, NE), BF16),
            pltpu.VMEM((11, 256, 256), BF16),
            pltpu.VMEM((2, 512, 512), BF16),
            pltpu.VMEM((512, 3 * LANES), BF16),
            pltpu.VMEM((66 * SLAB, NOBS), BF16),
            pltpu.VMEM((8, NOBS), F32),
            pltpu.VMEM((8, NOBS), F32),
            pltpu.SemaphoreType.DMA((NE,)),
            pltpu.SemaphoreType.DMA((NE,)),
            pltpu.SemaphoreType.DMA((NE,)),
            pltpu.SemaphoreType.DMA((NE,)),
            pltpu.SemaphoreType.DMA((NA * NB,)),
            pltpu.SemaphoreType.DMA((NA * NB,)),
            pltpu.SemaphoreType.DMA((NE,)),
            pltpu.SemaphoreType.DMA((NE,)),
            pltpu.SemaphoreType.DMA((2,)),
        ],
        compiler_params=pltpu.CompilerParams(
            collective_id=1, has_side_effects=True, vmem_limit_bytes=32 * 1024 * 1024
        ),
        name="cycle",
    )(x, cw, cb.reshape(1, 256), ow.T, oi, oc, ov, og, hcol_s, hrow, hcol)


def solution(mesh):
    return jax.shard_map(
        per_device,
        mesh=mesh,
        in_specs=(
            P("ens", None, "lat", "lon"),
            P(),
            P(),
            P(),
            P("lat", "lon", None),
            P("lat", "lon"),
            P("lat", "lon", None),
            P("lat", "lon", None),
        ),
        out_specs=P("ens", None, "lat", "lon"),
        check_vma=False,
    )
```
